32 devices in a mesh: expert: 8 (over z, y), vocab: 4 (over x, core).
Axes of the slice: x: 2, y: 2, z: 4, core: 2. Of those that a mesh axis runs over, the one named last changes fastest.
Arguments:
- layer_out: bfloat16 [256, 2048], P('expert'), may hold values from -6 to 6
- moe_input: bfloat16 [256, 2048], P('expert'), may hold values from -6 to 6
- final_gain: float32 [2048], replicated, may hold values from 0.1 to 1.9
- head_weight: bfloat16 [2048, 12288], P(None, ('expert', 'vocab')), may hold values from -0.125 to 0.125
- clean_ids: int32 [256], P('expert'), may hold values from 0 to 12287
- levels: int32 [256], P('expert'), may hold values from 0 to 15
- ratio_table: float32 [16], replicated, may hold values from 0.5 to 8
- gate_weights: float32 [256, 8], P('expert'), may hold values from 0.05 to 0.5
- expert_ids: int32 [256, 8], P('expert'), may hold values from 0 to 15, all different within a row; in each aligned block of 32 rows (0 to 31, 32 to 63, ...) at most 32 rows name the same one
- w_gate: bfloat16 [16, 2048, 1024], P('expert', None, 'vocab'), may hold values from -0.125 to 0.125
- w_up: bfloat16 [16, 2048, 1024], P('expert', None, 'vocab'), may hold values from -0.125 to 0.125
- w_down: bfloat16 [16, 1024, 2048], P('expert', 'vocab'), may hold values from -0.1875 to 0.1875
Outputs:
- head_grad: float32 [2048, 12288], P(None, ('expert', 'vocab'))
- residual_grad: float32 [256, 2048], P('expert', 'vocab')
- input_grad: float32 [256, 2048], P('expert', 'vocab')
The draws below stay inside these ranges and needn't reach their ends.
Inputs may be any that keep to these rules, and one draw needn't show every extreme that they name: `expert_ids`: the 8 experts of a row are distinct; among the 32 rows of one index of expert no expert is named by more than 32 rows.
All inputs are finite; a program needn't handle non-finite values.
Results may differ from the reference program's by a relative error of at most 0.0044.
The reference program's roundings to bfloat16 on the way (of `normed`, `score_grad` and `routed_grad`) count: a program that leaves them out, or rounds other values in their place, can miss the bound.
Values may be sent and summed in bfloat16 or wider, within the bound.
A program may use at most 64 MiB of HBM per device.

```python
import math
import jax
import jax.numpy as jnp
import numpy as np
from jax import lax

D = 2048
FF = 1024
TOP = 8
VOC_DEV = 384
ROWS_DEV = 32
LEVELS = 16
EXPERTS = 16
VOCAB = 12288
ROWS = 256
CAP = 32
N_EXPERT = 8
N_VOCAB = 4


def with_ends(values, key, low, top_value):
    spot = [jax.random.randint(jax.random.fold_in(key, axis), (), 0, length) for axis, length in enumerate(values.shape)]
    widest = values.shape.index(max(values.shape))
    next_to = spot[:widest] + [(spot[widest] + 1) % values.shape[widest]] + spot[widest + 1:]
    return values.at[tuple(spot)].set(low).at[tuple(next_to)].set(top_value)


def block_levels(rng, shape, shards, smallest, top_value):
    gain, own = 1.0, jax.random.fold_in(rng, 6)
    for dim, parts in shards:
        draws = jnp.exp(jax.random.uniform(jax.random.fold_in(own, dim), (parts,), jnp.float32, smallest / len(shards), top_value / len(shards)))
        gain = gain * jnp.repeat(draws, shape[dim] // parts).reshape([-1 if axis == dim else 1 for axis in range(len(shape))])
    return gain


def cumulative_ranks(amount, slope):
    portions = [(1 << 20) // math.isqrt(standing ** slope) + 1 for standing in range(1, amount + 1)]
    scale = 1 + sum(portions) // (1 << 30)
    return np.cumsum(np.array([max(1, weight // scale) for weight in portions]))


def ranked(key, extent, count, skew):
    listing = cumulative_ranks(count, skew)
    ticket = jax.random.randint(jax.random.fold_in(key, 1), extent, 0, int(listing[count - 1]))
    rank = jnp.searchsorted(jnp.asarray(listing, jnp.int32), ticket, side="right")
    return jax.random.permutation(jax.random.fold_in(key, 2), count)[rank].astype(jnp.int32)


def assign_block(key, own, number, rows, amount, top, most, skew):
    sequence = jax.random.permutation(key, amount)
    packed, ordinary = shares(amount, rows * top, most, skew, True), shares(amount, rows * top, most, skew, False)
    places = jnp.arange(amount)

    def named(lengths, rotation):
        used = int((lengths > 0).sum())
        fixed = max(1, used // 4)
        shifted = fixed + (places - fixed + rotation * (used - fixed)) % max(1, amount - fixed)
        return jnp.zeros((amount,), jnp.int32).at[sequence[jnp.where(places < fixed, places, shifted)]].set(jnp.asarray(lengths, jnp.int32))

    lengths = jnp.where(number % 4 == 0, named(packed, number // 4), named(ordinary, number - number // 4 - 1))
    mixed = jax.random.permutation(jax.random.fold_in(own, 3), amount)
    donor, receiver = mixed[0:amount // 2 * 2:2], mixed[1:amount // 2 * 2:2]
    room = jnp.minimum(lengths[donor] - 1, most - lengths[receiver]) // 2
    room = jnp.where((donor == sequence[0]) | (receiver == sequence[0]) | (lengths[receiver] == 0), 0, jnp.maximum(room, 0))
    shifted = jax.random.randint(jax.random.fold_in(own, 4), (amount // 2,), 0, 1 << 20) % (room + 1)
    lengths = lengths.at[donor].add(-shifted).at[receiver].add(shifted)
    items = jnp.searchsorted(jnp.cumsum(lengths), jnp.arange(rows * top), side="right").astype(jnp.int32)
    listing = items.reshape(top, rows).T
    listing = listing[jax.random.permutation(jax.random.fold_in(own, 1), rows)]
    rotation = jax.random.randint(jax.random.fold_in(own, 2), (rows, 1), 0, top)
    return jnp.take_along_axis(listing, (jnp.arange(top)[None, :] + rotation) % top, axis=1)


def shares(count, total, reach, lean, full):
    loads = [(1 << 20) // math.isqrt(grade ** lean) + 1 for grade in range(1, count + 1)]
    largest = reach if full else min(reach, max(-(-total // count), total * loads[0] // sum(loads)))
    least = 1 if total - largest >= count - 1 else 0
    holding, surplus = [largest] + [least] * (count - 1), total - largest - least * (count - 1)
    while surplus > 0:
        free = [i for i in range(1, count) if holding[i] < largest] or [i for i in range(1, count) if holding[i] < reach]
        pool, budget = sum([loads[i] for i in free]), surplus
        for i in free:
            extra = min(reach - holding[i], max(1, budget * loads[i] // pool), surplus)
            holding[i] = holding[i] + extra
            surplus = surplus - extra
    return np.array(holding)


def noise(stream_key, shape, spread, limit, shards=(), kind=jnp.bfloat16):
    entries = jax.random.normal(stream_key, shape, jnp.float32) * spread
    if len(shards) > 0:
        entries = block_levels(stream_key, shape, shards, -0.22, 0.18) * entries
    return jnp.clip(entries, min=-limit, max=limit).astype(kind)


def setup_inputs(seed: int = 0) -> dict:
    streams_of = jax.random.split(jax.random.key(seed), 13)
    layer_out = noise(streams_of[0], (ROWS, D), 1.0, 6.0, ((0, 8),))
    moe_input = noise(streams_of[1], (ROWS, D), 1.0, 6.0, ((0, 8),))
    final_gain = jnp.clip(1.0 + 0.18 * jax.random.normal(streams_of[2], (D,), jnp.float32), 0.1, 1.9)
    head_weight = noise(streams_of[3], (D, VOCAB), D ** -0.5, 0.125, ((1, 32),))
    clean_ids = with_ends(ranked(streams_of[4], (ROWS,), VOCAB, 2), jax.random.fold_in(streams_of[4], 3), 0, VOCAB - 1).astype(jnp.int32)
    levels = with_ends(jax.random.randint(streams_of[5], (ROWS,), 0, LEVELS), jax.random.fold_in(streams_of[5], 1), 0, LEVELS - 1).astype(jnp.int32)
    ratio_table = jnp.clip(jnp.exp(jax.random.uniform(streams_of[6], (LEVELS,), jnp.float32, math.log(0.5), math.log(8.0))), 0.5, 8.0)
    gate_weights = jnp.clip(jnp.exp(math.log(0.5) - 2.3025851 * jax.random.uniform(streams_of[7], (ROWS, TOP), jnp.float32) ** block_levels(streams_of[7], (ROWS, TOP), ((0, 8),), -0.2, 0.2)), 0.05, 0.5)
    expert_ids_keys = jax.random.split(jax.random.fold_in(streams_of[8], 1), ROWS // ROWS_DEV)
    expert_ids_turns = jax.random.permutation(jax.random.fold_in(streams_of[8], 3), ROWS // ROWS_DEV)
    expert_ids = jax.vmap(lambda own, number: assign_block(jax.random.fold_in(streams_of[8], 2), own, number, ROWS_DEV, EXPERTS, TOP, CAP, 2))(expert_ids_keys, expert_ids_turns).reshape((ROWS, TOP))
    w_gate = noise(streams_of[9], (EXPERTS, D, FF), D ** -0.5, 0.125, ((0, 8), (2, 4)))
    w_up = noise(streams_of[10], (EXPERTS, D, FF), D ** -0.5, 0.125, ((0, 8), (2, 4)))
    w_down = noise(streams_of[11], (EXPERTS, FF, D), FF ** -0.5, 0.1875, ((0, 8), (1, 4)))
    return {"layer_out": layer_out, "moe_input": moe_input, "final_gain": final_gain, "head_weight": head_weight, "clean_ids": clean_ids, "levels": levels, "ratio_table": ratio_table, "gate_weights": gate_weights, "expert_ids": expert_ids, "w_gate": w_gate, "w_up": w_up, "w_down": w_down}


epsilon = 1e-05

def slot_positions(expert_ids):
    id_blocks = expert_ids.reshape(N_EXPERT, ROWS_DEV * TOP)
    labels = jnp.arange(EXPERTS, dtype=jnp.int32)
    onehot = (id_blocks[:, :, None] == labels[None, None, :]).astype(jnp.int32)
    earlier = jnp.cumsum(onehot, axis=1) - onehot
    slot_index = lax.optimization_barrier(jnp.sum(earlier * onehot, axis=2))
    source = jnp.arange(N_EXPERT, dtype=jnp.int32)[:, None]
    position = id_blocks * (N_EXPERT * CAP) + source * CAP + slot_index
    return position.reshape(-1).astype(jnp.int32)

def expert_backward(operands):
    inputs_slot, grads_slot, gate_matrix, up_matrix, down_matrix = operands
    inputs_wide = inputs_slot.astype(jnp.float32)
    gate_pre = jnp.dot(inputs_wide, gate_matrix.astype(jnp.float32), preferred_element_type=jnp.float32)
    up_pre = jnp.dot(inputs_wide, up_matrix.astype(jnp.float32), preferred_element_type=jnp.float32)
    act_grad = jnp.dot(grads_slot.astype(jnp.float32), down_matrix.astype(jnp.float32).T, preferred_element_type=jnp.float32)
    sigmoid_gate = jax.nn.sigmoid(gate_pre)
    gate_grad = (act_grad * up_pre * sigmoid_gate * (1.0 + gate_pre * (1.0 - sigmoid_gate))).astype(jnp.bfloat16)
    up_grad = (act_grad * gate_pre * sigmoid_gate).astype(jnp.bfloat16)
    first = jnp.dot(gate_grad.astype(jnp.float32), gate_matrix.astype(jnp.float32).T, preferred_element_type=jnp.float32)
    second = jnp.dot(up_grad.astype(jnp.float32), up_matrix.astype(jnp.float32).T, preferred_element_type=jnp.float32)
    return first + second

def reference(layer_out, moe_input, final_gain, head_weight, clean_ids, levels, ratio_table, gate_weights, expert_ids, w_gate, w_up, w_down):
    values = layer_out.astype(jnp.float32)
    row_scale = jnp.sqrt(lax.optimization_barrier(jnp.mean(values * values, axis=1, keepdims=True)) + epsilon)
    unit_rows = values / row_scale
    normed = (unit_rows * final_gain[None, :]).astype(jnp.bfloat16)
    normed_wide = normed.astype(jnp.float32)
    ratio_rows = ratio_table[levels]
    loss_scale = 1.0 / math.sqrt(ROWS)
    block_count = N_EXPERT * N_VOCAB
    weight_blocks = head_weight.reshape(D, block_count, VOC_DEV).transpose(1, 0, 2)

    def scan_step(accumulated, block_input):
        weight_block, block_index = block_input
        weight_wide = weight_block.astype(jnp.float32)
        scores = jnp.dot(normed_wide, weight_wide, preferred_element_type=jnp.float32)
        columns = block_index * VOC_DEV + jnp.arange(VOC_DEV, dtype=jnp.int32)
        target_hit = (clean_ids[:, None] == columns[None, :]).astype(jnp.float32)
        score_grad = ((jnp.exp(scores) - ratio_rows[:, None] * target_hit) * loss_scale).astype(jnp.bfloat16)
        grad_wide = score_grad.astype(jnp.float32)
        block_grad = jnp.dot(normed_wide.T, grad_wide, preferred_element_type=jnp.float32)
        accumulated = accumulated + jnp.dot(grad_wide, weight_wide.T, preferred_element_type=jnp.float32)
        return (accumulated, block_grad)
    normed_grad, grad_blocks = lax.scan(scan_step, jnp.zeros((ROWS, D), jnp.float32), (weight_blocks, jnp.arange(block_count, dtype=jnp.int32)))
    head_grad = grad_blocks.transpose(1, 0, 2).reshape(D, VOCAB)
    gained = final_gain[None, :] * normed_grad
    residual_grad = (gained - unit_rows * lax.optimization_barrier(jnp.mean(unit_rows * gained, axis=1, keepdims=True))) / row_scale
    routed_grad = (gate_weights[:, :, None] * residual_grad[:, None, :]).astype(jnp.bfloat16).reshape(ROWS * TOP, D)
    inputs_rep = jnp.repeat(moe_input, TOP, axis=0)
    position = slot_positions(expert_ids)
    buffer_rows = EXPERTS * N_EXPERT * CAP
    inputs_buffer = jnp.zeros((buffer_rows, D), jnp.bfloat16).at[position].set(inputs_rep)
    grads_buffer = jnp.zeros((buffer_rows, D), jnp.bfloat16).at[position].set(routed_grad)
    slot_grads = lax.map(expert_backward, (inputs_buffer.reshape(EXPERTS, N_EXPERT * CAP, D), grads_buffer.reshape(EXPERTS, N_EXPERT * CAP, D), w_gate, w_up, w_down))
    per_pair = slot_grads.reshape(buffer_rows, D)[position]
    input_grad = lax.optimization_barrier(jnp.sum(per_pair.reshape(ROWS, TOP, D), axis=1))
    return (head_grad, residual_grad, input_grad)
```

```python
import functools
import math

import jax
import jax.numpy as jnp
from jax import lax
from jax.experimental import pallas as pl
from jax.experimental.pallas import tpu as pltpu
from jax.sharding import PartitionSpec as P

epsilon = 1e-05
CORES = 2
PAIR = 2
WIDE = 512
MESH = pl.DeviceIdType.MESH
VMEM = pl.BlockSpec(memory_space=pltpu.VMEM)
SMEM = pl.BlockSpec(memory_space=pltpu.SMEM)
ANY = pl.BlockSpec(memory_space=pl.ANY)
f32, bf16 = jnp.float32, jnp.bfloat16
TRANSPOSED = (((1,), (1,)), ((), ()))


def flip(x, mask):
    bit = 1
    while bit <= mask:
        if mask & bit:
            x = x + bit - 2 * bit * ((x // bit) % 2)
        bit *= 2
    return x


def remote(src, dst, send, recv, target):
    return pltpu.make_async_remote_copy(
        src_ref=src, dst_ref=dst, send_sem=send, recv_sem=recv, device_id=target,
        device_id_type=MESH,
    )


def step_kernel(
    layer_ref, moe_ref, gain_ref, head_ref, clean_ref, level_ref, table_ref, gates_ref, ids_ref,
    gate_hbm, up_hbm, down_hbm,
    normed_out, sg_out, residual_out, input_out,
    normed_all, moe_all, res_all, meta_all, meta_t, head, w_gate, w_up, w_down, sg, part, part_0,
    fac_gate, fac_up, y_send, y_recv, z_send, z_recv, own, x_send_1, x_recv_1, x_send_2, x_recv_2,
    res_wide, in_wide, unit, scale,
    ag_send, ag_recv, sib_send, sib_recv, grp_send, grp_recv, p0_send, p0_recv, one_send, one_recv,
    rs_send, rs_recv, x_send_sem, x_recv_sem, local_sem,
):
    e, v = lax.axis_index("expert"), lax.axis_index("vocab")
    n_e, n_v = lax.axis_size("expert"), lax.axis_size("vocab")
    a, c, n_a = v // CORES, v % CORES, n_v // CORES
    o, i, n_o = e // PAIR, e % PAIR, n_e // PAIR
    rows, width = layer_ref.shape
    total_rows = rows * n_e
    vocab_local = head_ref.shape[1]
    local_experts, _, hidden = gate_hbm.shape
    experts_all = local_experts * n_e
    share = width // n_v
    n_g = n_o // 2
    group = 4 * rows
    n_cc = width // WIDE

    def device(o_at, i_at, a_at):
        return (o_at * PAIR + i_at, a_at * CORES + c)

    sibling = (e, a * CORES + 1 - c)
    outer_peer = [device(flip(o, m), i, a) for m in range(n_o)]
    inner_peer = device(o, 1 - i, a)
    chip_peer = [device(o, i, lax.rem(a + d, n_a)) for d in range(n_a)]

    barrier = pltpu.get_barrier_semaphore()
    others = outer_peer[1:] + [inner_peer] + chip_peer[1:] + [sibling]
    for other in others:
        pl.semaphore_signal(barrier, inc=1, device_id=other, device_id_type=MESH)

    def block(m, across):
        at = flip(o, m) * PAIR + (1 - i if across else i)
        return pl.ds(pl.multiple_of(at * rows, rows), rows)

    def group_rows(g):
        return pl.ds(pl.multiple_of(flip(o // 2, g) * group, group), group)

    sends = []

    def start(copy):
        copy.start()
        sends.append(copy)

    def landed(ref, recv):
        remote(ref, ref, recv, recv, sibling).wait_recv()

    def spread(kind, buf, across, m):
        ref = buf.at[block(m, False)]
        if across:
            start(remote(ref, ref, ag_send.at[kind, 1, m], ag_recv.at[kind, 1, m], inner_peer))
        else:
            start(remote(buf.at[block(0, False)], buf.at[block(0, False)], ag_send.at[kind, 0, m],
                         ag_recv.at[kind, 0, m], outer_peer[m]))

    def spread_own(kind, buf):
        for m in range(1, n_o):
            spread(kind, buf, False, m)
            if m == 1:
                spread(kind, buf, True, 0)

    def forward(kind, buf, m):
        landed(buf.at[block(m, False)], ag_recv.at[kind, 0, m])
        spread(kind, buf, True, m)

    def crossed(kind, buf, m):
        landed(buf.at[block(m, True)], ag_recv.at[kind, 1, m])

    def to_sibling(kind, buf, m, across):
        ref, at = buf.at[block(m, across)], 2 * m + across
        start(remote(ref, ref, sib_send.at[kind, at], sib_recv.at[kind, at], sibling))

    def from_sibling(kind, buf, m, across):
        at = 2 * m + across
        landed(buf.at[block(m, across)], sib_recv.at[kind, at])

    loads = [
        pltpu.make_async_copy(gate_hbm, w_gate, local_sem.at[0]),
        pltpu.make_async_copy(up_hbm, w_up, local_sem.at[1]),
        pltpu.make_async_copy(down_hbm, w_down, local_sem.at[2]),
    ]

    def factors(k):
        lane = lax.broadcasted_iota(jnp.int32, (1, meta_all.shape[1]), 1)
        step = math.gcd(total_rows, 256)
        for r in range(0, total_rows, step):
            at = pl.ds(r, step)
            x = moe_all[at, :]
            gate_pre = jnp.dot(x, w_gate[k], preferred_element_type=f32)
            up_pre = jnp.dot(x, w_up[k], preferred_element_type=f32)
            weight = jnp.sum(jnp.where(lane == e * local_experts + k, meta_all[at, :], 0.0),
                             axis=1, keepdims=True)
            s = jax.nn.sigmoid(gate_pre)
            fac_gate[k, at, :] = weight * (up_pre * s * (1.0 + gate_pre * (1.0 - s)))
            fac_up[k, at, :] = weight * (gate_pre * s)

    def hidden_grads(g):
        at = group_rows(g)
        x = res_all[at, :]
        grads = []
        for k in range(local_experts):
            act = lax.dot_general(x, w_down[k], TRANSPOSED, preferred_element_type=f32)
            grads.append((act * fac_gate[k, at, :]).astype(bf16))
            grads.append((act * fac_up[k, at, :]).astype(bf16))
        return grads

    def input_terms(g, grads, j):
        columns = pl.ds(j * WIDE, WIDE)
        term = None
        for k in range(local_experts):
            for grad, weight in ((grads[2 * k], w_gate), (grads[2 * k + 1], w_up)):
                more = lax.dot_general(grad, weight[k, columns, :], TRANSPOSED,
                                       preferred_element_type=f32)
                term = more if term is None else term + more
        part[group_rows(g), columns] = term

    def p0_copy(g, j):
        at, columns = group_rows(g), pl.ds(j * WIDE, WIDE)
        return remote(part.at[at, columns], part_0.at[at, columns], p0_send.at[g, j],
                      p0_recv.at[g, j], sibling)

    def normed_copy(g):
        at = group_rows(g)
        return remote(normed_all.at[at], normed_out.at[at], grp_send.at[0, g], grp_recv.at[0, g],
                      sibling)

    def sg_copy(g):
        at = group_rows(g)
        return remote(sg.at[at, pl.ds(0, vocab_local)], sg_out.at[at], grp_send.at[1, g],
                      grp_recv.at[1, g], sibling)

    head_copy = remote(head_ref, head.at[:, pl.ds(0, vocab_local)], one_send.at[0],
                       one_recv.at[0], sibling)
    meta_copy = remote(meta_all, meta_all, one_send.at[1], one_recv.at[1], sibling)

    def column_share(core):
        return pl.ds(pl.multiple_of((a * CORES + core) * share, share), share)

    residual_copy = remote(res_wide.at[:, column_share(0)], residual_out, one_send.at[2],
                           one_recv.at[2], sibling)
    input_copy = remote(in_wide.at[:, pl.ds(0, share)], input_out, one_send.at[3],
                        one_recv.at[3], sibling)

    @pl.when(c == CORES - 1)
    def _():
        own_head = pltpu.make_async_copy(head_ref, head.at[:, pl.ds(vocab_local, vocab_local)],
                                         local_sem.at[3])
        own_head.start()
        values = layer_ref[...].astype(f32)
        row_scale = jnp.sqrt(jnp.sum(values * values, axis=1, keepdims=True) / width + epsilon)
        unit_rows = values / row_scale
        normed_all[block(0, False), :] = (unit_rows * gain_ref[...]).astype(bf16)
        unit[...] = unit_rows
        scale[...] = jnp.broadcast_to(row_scale, scale.shape)
        meta_t[...] = jnp.zeros_like(meta_t)
        label = lax.broadcasted_iota(jnp.int32, (experts_all, rows), 0)
        gates = jnp.zeros((experts_all, rows), f32)
        for k in range(ids_ref.shape[0]):
            gates = gates + jnp.where(ids_ref[k:k + 1, :] == label, gates_ref[k:k + 1, :], 0.0)
        ratio = jnp.zeros((1, rows), f32)
        for k in range(table_ref.shape[0]):
            ratio = ratio + jnp.where(level_ref[...] == k, table_ref[k], 0.0)
        meta_t[0:experts_all, 0:rows] = gates
        meta_t[experts_all:experts_all + 1, 0:rows] = ratio
        meta_t[experts_all + 1:experts_all + 2, 0:rows] = clean_ref[...].astype(f32)
        meta_all[block(0, False), :] = jnp.transpose(meta_t[...])[0:rows, :]
        pl.semaphore_wait(barrier, len(others))

        spread_own(1, meta_all)
        spread_own(0, normed_all)
        for load in loads:
            load.start()

        def scores(g):
            at = group_rows(g)
            x = normed_all[at, :]
            meta = meta_all[at, :]
            ratio = meta[:, experts_all:experts_all + 1]
            clean = meta[:, experts_all + 1:experts_all + 2]
            wide = math.gcd(2 * vocab_local, 256)
            first = (e * n_v + a * CORES) * vocab_local
            for n in range(0, 2 * vocab_local, wide):
                columns = pl.ds(n, wide)
                score = jnp.dot(x, head[:, columns], preferred_element_type=f32)
                label = first + n + lax.broadcasted_iota(jnp.int32, (1, wide), 1)
                hit = jnp.where(clean == label.astype(f32), ratio, 0.0)
                sg[at, columns] = ((jnp.exp(score) - hit) * (1.0 / math.sqrt(total_rows))).astype(bf16)

        def head_terms(g):
            at = group_rows(g)
            x = sg[at, :]
            for j in range(n_cc):
                columns = pl.ds(j * WIDE, WIDE)
                part[at, columns] = lax.dot_general(x, head[columns, :], TRANSPOSED,
                                                    preferred_element_type=f32)

        def y_copy(q, m):
            return remote(y_send.at[q, m], y_recv.at[q, m], rs_send.at[q, 0, m],
                          rs_recv.at[q, 0, m], inner_peer)

        def z_copy(q, m):
            return remote(z_send.at[q, m], z_recv.at[q, m], rs_send.at[q, 1, m],
                          rs_recv.at[q, 1, m], outer_peer[m])

        def chip_term(q, m, across):
            at = block(m, across)
            return part[at, :] + part_0[at, :] if q else part[at, :]

        def y_step(q, m):
            y_send[q, m] = chip_term(q, m, True).astype(bf16)
            start(y_copy(q, m))

        def z_step(q, m):
            y_copy(q, m).wait_recv()
            term = chip_term(q, m, False) + y_recv[q, m].astype(f32)
            if m:
                z_send[q, m] = term.astype(bf16)
                start(z_copy(q, m))
            else:
                own[...] = term

        def z_sum(q):
            term = own[...]
            for m in range(1, n_o):
                z_copy(q, m).wait_recv()
                term = term + z_recv[q, m].astype(f32)
            return term

        forward(1, meta_all, 1)
        forward(0, normed_all, 1)
        for m in range(2, n_o):
            forward(1, meta_all, m)
        for m in range(n_o):
            crossed(1, meta_all, m)
        start(meta_copy)
        own_head.wait()
        landed(head.at[:, pl.ds(0, vocab_local)], one_recv.at[0])
        ahead = 2
        if ahead < n_o:
            forward(0, normed_all, ahead)
            ahead += 1
        for g in range(n_g):
            for m in (2 * g, 2 * g + 1):
                crossed(0, normed_all, m)
            start(normed_copy(g))
            scores(g)
            start(sg_copy(g))
            for _ in range(2):
                if ahead < n_o:
                    forward(0, normed_all, ahead)
                    ahead += 1
            head_terms(g)
            for m in (2 * g, 2 * g + 1):
                y_step(0, m)
        for m in list(range(1, n_o)) + [0]:
            z_step(0, m)
        keep = [
            pltpu.make_async_copy(normed_all, normed_out, local_sem.at[4]),
            pltpu.make_async_copy(sg.at[:, pl.ds(vocab_local, vocab_local)], sg_out,
                                  local_sem.at[5]),
        ]
        for copy in keep:
            copy.start()
        x_send_1[...] = z_sum(0)
        chips = []
        for d in range(1, n_a):
            copy = remote(x_send_1, x_recv_1.at[d], x_send_sem.at[0, d], x_recv_sem.at[0, d],
                          chip_peer[d])
            start(copy)
            chips.append(copy)
        for load in loads:
            load.wait()
        normed_grad = x_send_1[...]
        for d, copy in enumerate(chips):
            copy.wait_recv()
            normed_grad = normed_grad + x_recv_1[d + 1]
        gained = gain_ref[...] * normed_grad
        mean = jnp.sum(unit[...] * gained, axis=1, keepdims=True) / width
        residual = (gained - unit[...] * mean) / scale[:, 0:1]
        res_all[block(0, False), :] = residual.astype(bf16)
        res_wide[...] = residual
        spread_own(3, res_all)
        to_sibling(1, res_all, 0, False)
        start(residual_copy)
        residual_out[...] = res_wide[:, column_share(1)]
        for m in range(n_o):
            for across in (False, True):
                from_sibling(0, moe_all, m, across)
        half = max(local_experts // 2, 1)
        for k in range(half):
            factors(k)

        def arrive(m):
            forward(3, res_all, m)
            to_sibling(1, res_all, m, False)

        def arrive_across(m):
            crossed(3, res_all, m)
            to_sibling(1, res_all, m, True)

        arrive(1)
        for k in range(half, local_experts):
            factors(k)
        ahead = 2
        if ahead < n_o:
            arrive(ahead)
            ahead += 1
        for g in range(n_g):
            for m in (2 * g, 2 * g + 1):
                arrive_across(m)
            grads = hidden_grads(g)
            for _ in range(2):
                if ahead < n_o:
                    arrive(ahead)
                    ahead += 1
            for j in range(n_cc):
                input_terms(g, grads, j)
            for j in range(n_cc):
                p0_copy(g, j).wait_recv()
            for m in (2 * g, 2 * g + 1):
                y_step(1, m)
        for m in list(range(1, n_o)) + [0]:
            z_step(1, m)
        x_send_2[...] = z_sum(1)
        chips = []
        for d in range(1, n_a):
            at = lax.rem(a + d, n_a)
            columns = pl.ds(pl.multiple_of(at * CORES * share, share), CORES * share)
            copy = remote(x_send_2.at[:, columns], x_recv_2.at[d], x_send_sem.at[1, d],
                          x_recv_sem.at[1, d], chip_peer[d])
            start(copy)
            chips.append(copy)
        total = x_send_2[:, pl.ds(pl.multiple_of(a * CORES * share, share), CORES * share)]
        for d, copy in enumerate(chips):
            copy.wait_recv()
            total = total + x_recv_2[d + 1]
        in_wide[...] = total
        start(input_copy)
        input_out[...] = in_wide[:, pl.ds(share, share)]
        for copy in keep:
            copy.wait()
        for copy in sends:
            copy.wait_send()

    @pl.when(c == 0)
    def _():
        sends.clear()
        own_moe = pltpu.make_async_copy(moe_ref, moe_all.at[block(0, False)], local_sem.at[3])
        own_moe.start()
        for load in loads:
            load.start()
        pl.semaphore_wait(barrier, len(others))
        start(head_copy)
        for g in range(n_g):
            landed(normed_out.at[group_rows(g)], grp_recv.at[0, g])
        own_moe.wait()
        spread_own(2, moe_all)
        to_sibling(0, moe_all, 0, False)
        for m in range(1, n_o):
            forward(2, moe_all, m)
            to_sibling(0, moe_all, m, False)
        for m in range(n_o):
            crossed(2, moe_all, m)
            to_sibling(0, moe_all, m, True)
        for load in loads:
            load.wait()
        landed(meta_all, one_recv.at[1])
        for k in range(local_experts):
            factors(k)
        for g in range(n_g):
            landed(sg_out.at[group_rows(g)], grp_recv.at[1, g])
        for g in range(n_g):
            for m in (2 * g, 2 * g + 1):
                for across in (False, True):
                    from_sibling(1, res_all, m, across)
            grads = hidden_grads(g)
            for j in range(n_cc):
                input_terms(g, grads, j)
                start(p0_copy(g, j))
        landed(residual_out, one_recv.at[2])
        landed(input_out, one_recv.at[3])
        for copy in sends:
            copy.wait_send()


def step(layer_out, moe_input, gain, head_weight, clean, levels, table, gates, ids, w_gate, w_up,
         w_down):
    n_e, n_v = lax.axis_size("expert"), lax.axis_size("vocab")
    n_o, n_a = n_e // PAIR, n_v // CORES
    rows, width = layer_out.shape
    total_rows, share = rows * n_e, width // n_v
    vocab_local = head_weight.shape[1]
    local_experts, _, hidden = w_gate.shape
    lanes = -(-(local_experts * n_e + 2) // 128) * 128
    n_g, n_cc = n_o // 2, width // WIDE
    dma = pltpu.SemaphoreType.DMA
    scratch = [
        pltpu.VMEM((total_rows, width), bf16),
        pltpu.VMEM((total_rows, width), bf16),
        pltpu.VMEM((total_rows, width), bf16),
        pltpu.VMEM((total_rows, lanes), f32),
        pltpu.VMEM((lanes, 128), f32),
        pltpu.VMEM((width, 2 * vocab_local), bf16),
        pltpu.VMEM(w_gate.shape, bf16),
        pltpu.VMEM(w_up.shape, bf16),
        pltpu.VMEM(w_down.shape, bf16),
        pltpu.VMEM((total_rows, 2 * vocab_local), bf16),
        pltpu.VMEM((total_rows, width), f32),
        pltpu.VMEM((total_rows, width), f32),
        pltpu.VMEM((local_experts, total_rows, hidden), f32),
        pltpu.VMEM((local_experts, total_rows, hidden), f32),
        pltpu.VMEM((2, n_o, rows, width), bf16),
        pltpu.VMEM((2, n_o, rows, width), bf16),
        pltpu.VMEM((2, n_o, rows, width), bf16),
        pltpu.VMEM((2, n_o, rows, width), bf16),
        pltpu.VMEM((rows, width), f32),
        pltpu.VMEM((rows, width), f32),
        pltpu.VMEM((n_a, rows, width), f32),
        pltpu.VMEM((rows, width), f32),
        pltpu.VMEM((n_a, rows, CORES * share), f32),
        pltpu.VMEM((rows, width), f32),
        pltpu.VMEM((rows, CORES * share), f32),
        pltpu.VMEM((rows, width), f32),
        pltpu.VMEM((rows, 128), f32),
        dma((4, 2, n_o)), dma((4, 2, n_o)),
        dma((2, 2 * n_o)), dma((2, 2 * n_o)),
        dma((2, n_g)), dma((2, n_g)),
        dma((n_g, n_cc)), dma((n_g, n_cc)),
        dma((4,)), dma((4,)),
        dma((2, 2, n_o)), dma((2, 2, n_o)),
        dma((2, n_a)), dma((2, n_a)),
        dma((6,)),
    ]
    return pl.pallas_call(
        step_kernel,
        out_shape=[
            jax.ShapeDtypeStruct((total_rows, width), bf16),
            jax.ShapeDtypeStruct((total_rows, vocab_local), bf16),
            jax.ShapeDtypeStruct((rows, share), f32),
            jax.ShapeDtypeStruct((rows, share), f32),
        ],
        in_specs=[VMEM, ANY, VMEM, ANY, VMEM, VMEM, SMEM, VMEM, VMEM, ANY, ANY, ANY],
        out_specs=[ANY, ANY, VMEM, VMEM],
        scratch_shapes=scratch,
        compiler_params=pltpu.CompilerParams(
            collective_id=0, has_side_effects=True, vmem_limit_bytes=67043328,
        ),
    )(layer_out, moe_input, gain, head_weight, clean, levels, table, gates, ids, w_gate, w_up,
      w_down)


def on_device(
    layer_out,
    moe_input,
    final_gain,
    head_weight,
    clean_ids,
    levels,
    ratio_table,
    gate_weights,
    expert_ids,
    w_gate,
    w_up,
    w_down,
):
    normed_all, score_grad, residual_grad, input_grad = step(
        layer_out, moe_input, final_gain[None, :], head_weight, clean_ids[None, :],
        levels[None, :], ratio_table, gate_weights.T, expert_ids.T, w_gate, w_up, w_down,
    )
    head_grad = lax.dot_general(
        normed_all, score_grad, (((0,), (0,)), ((), ())), preferred_element_type=jnp.float32
    )
    return (head_grad, residual_grad, input_grad)


def solution(mesh):
    in_specs = (
        P("expert", None),
        P("expert", None),
        P(),
        P(None, ("expert", "vocab")),
        P("expert"),
        P("expert"),
        P(),
        P("expert", None),
        P("expert", None),
        P("expert", None, "vocab"),
        P("expert", None, "vocab"),
        P("expert", "vocab", None),
    )
    out_specs = (P(None, ("expert", "vocab")), P("expert", "vocab"), P("expert", "vocab"))
    return jax.shard_map(
        on_device, mesh=mesh, in_specs=in_specs, out_specs=out_specs, check_vma=False
    )
```

```python
import functools
import math

import jax
import jax.numpy as jnp
from jax import lax
from jax.experimental import pallas as pl
from jax.experimental.pallas import tpu as pltpu
from jax.sharding import PartitionSpec as P

epsilon = 1e-05
CORES = 2
PAIR = 2
TILE = 256
SPARE = 6 << 20
VMEM_BYTES = 67043328
MESH = pl.DeviceIdType.MESH
ANY = pl.BlockSpec(memory_space=pl.ANY)
VMEM = pl.BlockSpec(memory_space=pltpu.VMEM)
HBM = pl.BlockSpec(memory_space=pltpu.HBM)
f32, bf16 = jnp.float32, jnp.bfloat16
TRANSPOSED = (((1,), (1,)), ((), ()))
META, NORMED, MOE, RES = range(4)
KINDS = 5


def flip(x, mask):
    bit = 1
    while bit <= mask:
        if mask & bit:
            x = x + bit - 2 * bit * ((x // bit) % 2)
        bit *= 2
    return x


def remote(src, dst, send, recv, target):
    return pltpu.make_async_remote_copy(
        src_ref=src, dst_ref=dst, send_sem=send, recv_sem=recv, device_id=target,
        device_id_type=MESH,
    )


def step_kernel(
    layer_hbm, moe_hbm, gain_hbm, head_hbm, clean_hbm, level_hbm, table_hbm, gates_hbm, ids_hbm,
    gate_hbm, up_hbm, down_hbm,
    normed_out, sg_out, residual_out, input_out,
    layer, gain, clean_ids, levels, table, gates, ids,
    normed_all, moe_all, res_all, meta_all, meta_t, head, head_pair, w_both, w_down, act,
    pair_both, sg, sg_pair, grads, grads_pair, part, fac_gate, fac_up,
    xs0, xr0, ys0, yr0, xs1, xr1, ys1, yr1, z_send, z_recv, own, dot_wide, dot_send, dot_recv, dot_chip, dot_outer, scale, unit,
    z_ss, z_rs, y_ss, y_rs, x_ss, x_rs, sib_ss, sib_rs, one_ss, one_rs, wide_ss, wide_rs, pair_ss, pair_rs,
    xs0_s, xs0_r, ys0_s, ys0_r, xs1_s, xs1_r, ys1_s, ys1_r, rz_s, rz_r, dot_s, dot_r, local_sem,
):
    e, v = lax.axis_index("expert"), lax.axis_index("vocab")
    n_e, n_v = lax.axis_size("expert"), lax.axis_size("vocab")
    a, c, n_a = v // CORES, v % CORES, n_v // CORES
    o, i, n_o = e // PAIR, e % PAIR, n_e // PAIR
    rows, width = layer.shape
    total_rows = rows * n_e
    vocab_local = head_hbm.shape[1]
    local_experts, _, hidden = gate_hbm.shape
    experts_all = local_experts * n_e
    share = width // n_v
    cut = share // 2
    row_step = math.gcd(total_rows, 256)
    row_parts = [pl.ds(r, row_step) for r in range(0, total_rows, row_step)]

    def device(o_at, i_at, a_at):
        return (o_at * PAIR + i_at, a_at * CORES + c)

    sibling = (e, a * CORES + 1 - c)
    outer_peer = [device(flip(o, m), i, a) for m in range(n_o)]
    inner_peer = device(o, 1 - i, a)
    chip_at = [lax.rem(a + d, n_a) for d in range(n_a)]
    chip_from = [lax.rem(a + n_a - d, n_a) for d in range(n_a)]
    chip_peer = [device(o, i, chip_at[d]) for d in range(n_a)]
    diagonal_peer = [device(o, 1 - i, chip_at[d]) for d in range(n_a)]

    barrier = pltpu.get_barrier_semaphore()
    others = outer_peer[1:] + [inner_peer] + chip_peer[1:] + diagonal_peer[1:] + [sibling]
    for other in others:
        pl.semaphore_signal(barrier, inc=1, device_id=other, device_id_type=MESH)

    def block(m, across):
        at = flip(o, m) * PAIR + (1 - i if across else i)
        return pl.ds(pl.multiple_of(at * rows, rows), rows)

    def columns_of(at, core):
        return pl.ds(pl.multiple_of((at * CORES + core) * share, share), share)

    def cut_columns(at, s):
        return pl.ds(pl.multiple_of((at * CORES + c) * share + s * cut, cut), cut)

    sends = []

    def start(copy):
        copy.start()
        sends.append(copy)

    def landed(ref, recv):
        remote(ref, ref, recv, recv, sibling).wait_recv()

    def piece(kind, buf, m, across, at, core):
        if kind >= RES:
            first = (at * CORES + core) * share + (kind - RES) * cut
            return buf.at[block(m, across), pl.ds(pl.multiple_of(first, cut), cut)]
        return buf.at[block(m, across), columns_of(at, core)]

    def plane(kind, buf, m):
        ref = piece(kind, buf, m, False, a, c)
        start(remote(ref, ref, y_ss.at[kind, m], y_rs.at[kind, m], inner_peer))
        for d in range(1, n_a):
            if m or kind >= RES:
                start(remote(ref, ref, x_ss.at[kind, 2 * m, d], x_rs.at[kind, 2 * m, d],
                             chip_peer[d]))
            start(remote(ref, ref, x_ss.at[kind, 2 * m + 1, d], x_rs.at[kind, 2 * m + 1, d],
                         diagonal_peer[d]))

    def to_sibling(kind, buf, m, across, d):
        ref, at = piece(kind, buf, m, across, chip_from[d], c), 2 * m + across
        start(remote(ref, ref, sib_ss.at[kind, at, d], sib_rs.at[kind, at, d], sibling))

    def spread(kind, buf):
        ref = piece(kind, buf, 0, False, a, c)
        for m in range(1, n_o):
            start(remote(ref, ref, z_ss.at[kind, m], z_rs.at[kind, m], outer_peer[m]))
        plane(kind, buf, 0)
        if kind >= RES:
            to_sibling(kind, buf, 0, False, 0)

    def forward(kind, buf, m):
        landed(piece(kind, buf, m, False, a, c), z_rs.at[kind, m])
        plane(kind, buf, m)
        to_sibling(kind, buf, m, False, 0)

    def crossed(kind, buf, m):
        landed(piece(kind, buf, m, True, a, c), y_rs.at[kind, m])
        to_sibling(kind, buf, m, True, 0)
        for across in ((False, True) if m or kind >= RES else (True,)):
            for d in range(1, n_a):
                landed(piece(kind, buf, m, across, chip_from[d], c),
                       x_rs.at[kind, 2 * m + across, d])
                to_sibling(kind, buf, m, across, d)

    def from_sibling(kind, buf):
        for m in range(n_o):
            for across in ((False, True) if m or kind >= RES else (True,)):
                for d in range(n_a):
                    landed(piece(kind, buf, m, across, chip_from[d], 1 - c),
                           sib_rs.at[kind, 2 * m + across, d])

    def lanes_of(k, j, n=1):
        return pl.ds((2 * k + j) * hidden, n * hidden)

    down_loads = [
        (down_hbm.at[k], w_down.at[pl.ds(k * hidden, hidden), :]) for k in range(local_experts)
    ]
    own_weights = [
        (src.at[k], w_both.at[:, lanes_of(k, j)])
        for k in range(local_experts) for j, src in enumerate((gate_hbm, up_hbm))
    ]
    loads = [
        pltpu.make_async_copy(src, dst, local_sem.at[k])
        for k, (src, dst) in enumerate((
            (layer_hbm, layer), (gain_hbm, gain), (clean_hbm, clean_ids), (level_hbm, levels),
            (table_hbm, table), (gates_hbm, gates), (ids_hbm, ids), (head_hbm, head),
            (moe_hbm, moe_all.at[block(0, False)]), *down_loads, *own_weights))
    ]
    for copy in loads:
        copy.start()
    meta_t[...] = jnp.zeros_like(meta_t)
    for copy in loads[:7]:
        copy.wait()
    values = layer[...].astype(f32)
    row_scale = jnp.sqrt(jnp.sum(values * values, axis=1, keepdims=True) / width + epsilon)
    unit_rows = values / row_scale
    normed_all[block(0, False), :] = (unit_rows * gain[...]).astype(bf16)
    unit[...] = unit_rows
    scale[...] = jnp.broadcast_to(row_scale, scale.shape)
    label = lax.broadcasted_iota(jnp.int32, (experts_all, rows), 0)
    expert_gates = jnp.zeros((experts_all, rows), f32)
    for k in range(ids.shape[0]):
        expert_gates = expert_gates + jnp.where(ids[k:k + 1, :] == label, gates[k:k + 1, :], 0.0)
    ratio_row = jnp.zeros((1, rows), f32)
    for k in range(table.shape[1]):
        ratio_row = ratio_row + jnp.where(levels[...] == k, table[:, k:k + 1], 0.0)
    meta_t[0:experts_all, 0:rows] = expert_gates
    meta_t[experts_all:experts_all + 1, 0:rows] = ratio_row
    meta_t[experts_all + 1:experts_all + 2, 0:rows] = clean_ids[...].astype(f32)
    meta_all[block(0, False), :] = jnp.transpose(meta_t[...])[0:rows, :]
    pl.semaphore_wait(barrier, len(others))

    def meta_copy(way, m, across=False):
        ref = meta_all.at[block(0 if way == 0 else m, across)]
        if way == 0:
            return remote(ref, ref, z_ss.at[META, m], z_rs.at[META, m], outer_peer[m])
        if way == 1:
            return remote(ref, ref, y_ss.at[META, m], y_rs.at[META, m], inner_peer)
        at = 2 * m + across
        return remote(ref, ref, sib_ss.at[META, at, 0], sib_rs.at[META, at, 0], sibling)

    @pl.when(c == CORES - 1)
    def _():
        for m in range(1, n_o):
            meta_copy(0, m).start()
        meta_copy(1, 0).start()
    spread(NORMED, normed_all)
    head_copies = []
    pair_copies = []
    for d in range(n_a):
        theirs = columns_of(chip_at[d], 1 - c)
        head_copies.append(remote(head_hbm.at[theirs, :], head_pair.at[d], wide_ss.at[0, d],
                                  wide_rs.at[0, d], sibling))
        for k in range(local_experts):
            for j, src in enumerate((gate_hbm, up_hbm)):
                pair_copies.append(remote(
                    src.at[k, theirs, :], pair_both.at[d, :, lanes_of(k, j)],
                    pair_ss.at[d, 2 * k + j], pair_rs.at[d, 2 * k + j], sibling))
    for copy in head_copies + pair_copies:
        start(copy)

    def factors(k):
        lane = lax.broadcasted_iota(jnp.int32, (1, meta_all.shape[1]), 1)
        for at in row_parts:
            x = moe_all[at, :]
            gate_pre = jnp.dot(x, w_both[:, lanes_of(k, 0)], preferred_element_type=f32)
            up_pre = jnp.dot(x, w_both[:, lanes_of(k, 1)], preferred_element_type=f32)
            weight = jnp.sum(jnp.where(lane == e * local_experts + k, meta_all[at, :], 0.0),
                             axis=1, keepdims=True)
            s = jax.nn.sigmoid(gate_pre)
            fac_gate[k, at, :] = weight * (up_pre * s * (1.0 + gate_pre * (1.0 - s)))
            fac_up[k, at, :] = weight * (gate_pre * s)

    act_seen = []

    def act_terms(s, core):
        for d in range(n_a):
            first = pl.multiple_of((chip_at[d] * CORES + core) * share + s * cut, cut)
            columns = pl.ds(first, cut)
            for at in row_parts:
                term = lax.dot_general(res_all[at, columns], w_down[:, columns], TRANSPOSED,
                                       preferred_element_type=f32)
                if act_seen:
                    act[at, :] += term
                else:
                    act[at, :] = term
            act_seen.append(d)

    def hidden_grads(k):
        for at in row_parts:
            own_act = act[at, pl.ds(k * hidden, hidden)]
            grads[at, lanes_of(k, 0)] = (own_act * fac_gate[k, at, :]).astype(bf16)
            grads[at, lanes_of(k, 1)] = (own_act * fac_up[k, at, :]).astype(bf16)

    def grads_copy(k):
        return remote(grads.at[:, lanes_of(k, 0, 2)], grads_pair.at[:, lanes_of(k, 0, 2)],
                      wide_ss.at[1, k], wide_rs.at[1, k], sibling)

    def own_terms(q, d, s):
        columns = cut_columns(chip_at[d], s)
        left, right = (grads, w_both) if q else (sg, head)
        for at in row_parts:
            part[d, s, at, :] = lax.dot_general(left[at, :], right[columns, :], TRANSPOSED,
                                                preferred_element_type=f32)

    def pair_terms(q, d, s):
        columns = pl.ds(s * cut, cut)
        left, right = (grads_pair, pair_both) if q else (sg_pair, head_pair)
        for at in row_parts:
            part[d, s, at, :] += lax.dot_general(left[at, :], right[d, columns, :], TRANSPOSED,
                                                 preferred_element_type=f32)

    def scores():
        for at in row_parts:
            x = normed_all[at, :]
            meta = meta_all[at, :]
            ratio = meta[:, experts_all:experts_all + 1]
            clean = meta[:, experts_all + 1:experts_all + 2]
            score = jnp.dot(x, head[...], preferred_element_type=f32)
            label = (e * n_v + v) * vocab_local + lax.broadcasted_iota(
                jnp.int32, (1, vocab_local), 1)
            hit = jnp.where(clean == label.astype(f32), ratio, 0.0)
            grad = ((jnp.exp(score) - hit) * (1.0 / math.sqrt(total_rows))).astype(bf16)
            sg[at, :] = grad
            dot = jnp.sum(grad.astype(f32) * score, axis=1, keepdims=True)
            dot_wide[at, :] = jnp.broadcast_to(dot, (row_step, 128))
        dot_send[0] = jnp.transpose(dot_wide[...])[0:8, :]

    def x0(q, d):
        return remote(xs0.at[q, d - 1], xr0.at[q, d - 1], xs0_s.at[q, d], xs0_r.at[q, d],
                      chip_peer[d])

    def y0(q):
        return remote(ys0.at[q], yr0.at[q], ys0_s.at[q], ys0_r.at[q], inner_peer)

    def y1(q):
        return remote(ys1.at[q], yr1.at[q], ys1_s.at[q], ys1_r.at[q], inner_peer)

    def x1(q, d):
        return remote(xs1.at[q, d - 1], xr1.at[q, d - 1], xs1_s.at[q, d], xs1_r.at[q, d],
                      chip_peer[d])

    def z(q, s, m):
        return remote(z_send.at[q, s, m], z_recv.at[q, s, m], rz_s.at[q, s, m], rz_r.at[q, s, m],
                      outer_peer[m])

    def terms_and_first(q):
        for d in range(1, n_a):
            pair_terms(q, d, 0)
            xs0[q, d - 1] = part[d, 0].astype(bf16)
            start(x0(q, d))
        for d in range(n_a):
            pair_terms(q, d, 1)
            for m in range(n_o):
                ys1[q, d, m] = part[d, 1, block(m, True), :].astype(bf16)
        start(y1(q))
        pair_terms(q, 0, 0)

    def dot_copies(stage):
        src = dot_send.at[stage]
        if stage == 0:
            return [remote(src, dot_recv.at[0], dot_s.at[0, 0], dot_r.at[0, 0], sibling)]
        if stage == 1:
            return [remote(src, dot_chip.at[d - 1], dot_s.at[1, d], dot_r.at[1, d], chip_peer[d])
                    for d in range(1, n_a)]
        if stage == 2:
            return [remote(src, dot_recv.at[1], dot_s.at[2, 0], dot_r.at[2, 0], inner_peer)]
        return [remote(src, dot_outer.at[m], dot_s.at[3, m], dot_r.at[3, m], outer_peer[m])
                for m in range(1, n_o)]

    def dot_start(stage):
        for copy in dot_copies(stage):
            start(copy)

    def dot_sum(stage):
        for copy in dot_copies(stage):
            copy.wait_recv()
        total = dot_send[stage]
        if stage == 0:
            return total + dot_recv[0]
        if stage == 1:
            for d in range(1, n_a):
                total = total + dot_chip[d - 1]
            return total
        if stage == 2:
            return total + dot_recv[1]
        for m in range(1, n_o):
            total = total + dot_outer[m]
        return total

    def dot_next(stage):
        dot_send[stage + 1] = dot_sum(stage)
        dot_start(stage + 1)

    def second(q):
        for d in range(1, n_a):
            x0(q, d).wait_recv()
        if q == 0:
            dot_next(1)

        def sum_0(m, across):
            at = block(m, across)
            term = part[0, 0, at, :]
            for d in range(1, n_a):
                term = term + xr0[q, d - 1, at, :].astype(f32)
            return term

        for m in range(n_o):
            ys0[q, m] = sum_0(m, True).astype(bf16)
        start(y0(q))
        y1(q).wait_recv()

        def sum_1(d, m):
            return part[d, 1, block(m, False), :] + yr1[q, d, m].astype(f32)

        for d in range(1, n_a):
            for m in range(n_o):
                xs1[q, d - 1, m] = sum_1(d, m).astype(bf16)
            start(x1(q, d))
        return sum_0, sum_1

    def third(q, sum_0, sum_1):
        y0(q).wait_recv()
        if q == 0:
            dot_next(2)
        for m in list(range(1, n_o)) + [0]:
            term = sum_0(m, False) + yr0[q, m].astype(f32)
            if m:
                z_send[q, 0, m] = term
                start(z(q, 0, m))
            else:
                own[0] = term
        for d in range(1, n_a):
            x1(q, d).wait_recv()
        for m in list(range(1, n_o)) + [0]:
            term = sum_1(0, m)
            for d in range(1, n_a):
                term = term + xr1[q, d - 1, m].astype(f32)
            if m:
                z_send[q, 1, m] = term
                start(z(q, 1, m))
            else:
                own[1] = term

    def fourth(q, s):
        term = own[s]
        for m in range(1, n_o):
            z(q, s, m).wait_recv()
            term = term + z_recv[q, s, m]
        return term


    @pl.when(c == CORES - 1)
    def _():
        for m in range(1, n_o):
            landed(meta_all.at[block(m, False)], z_rs.at[META, m])
            meta_copy(1, m).start()
            meta_copy(2, m).start()
    for m in range(1, n_o):
        forward(NORMED, normed_all, m)
    loads[8].wait()
    spread(MOE, moe_all)
    for m in range(n_o):
        crossed(NORMED, normed_all, m)

    @pl.when(c == CORES - 1)
    def _():
        for m in range(n_o):
            landed(meta_all.at[block(m, True)], y_rs.at[META, m])
            meta_copy(2, m, True).start()
        for m in range(n_o):
            if m:
                meta_copy(0, m).wait_send()
                meta_copy(2, m).wait_send()
            meta_copy(1, m).wait_send()
            meta_copy(2, m, True).wait_send()
    for m in range(1, n_o):
        forward(MOE, moe_all, m)

    @pl.when(c == 0)
    def _():
        for m in range(n_o):
            for across in ((False, True) if m else (True,)):
                landed(meta_all.at[block(m, across)], sib_rs.at[META, 2 * m + across, 0])
    loads[7].wait()
    from_sibling(NORMED, normed_all)
    scores()
    sg_copy = remote(sg, sg_pair, one_ss.at[0], one_rs.at[0], sibling)
    start(sg_copy)
    dot_start(0)
    for d in range(n_a):
        for s in range(2):
            own_terms(0, d, s)
    for copy in head_copies:
        copy.wait_recv()
    sg_copy.wait_recv()
    dot_next(0)
    terms_and_first(0)
    for at in row_parts:
        for n in range(0, width, row_step):
            normed_out[pl.ds(n, row_step), at] = jnp.transpose(normed_all[at, pl.ds(n, row_step)])
    sg_out[...] = sg[...]
    sums = second(0)
    for copy in loads[9:]:
        copy.wait()
    third(0, *sums)
    for m in range(n_o):
        crossed(MOE, moe_all, m)
    from_sibling(MOE, moe_all)
    dot_total = dot_sum(3)
    dot_wide[...] = jnp.transpose(jnp.broadcast_to(dot_total[0:1, :], (128, total_rows)))
    mean = dot_wide[block(0, False), 0:1] / width
    own_gain = gain[:, columns_of(a, c)]
    own_unit = unit[:, columns_of(a, c)]
    for s in range(2):
        at = slice(s * cut, (s + 1) * cut)
        residual = (own_gain[:, at] * fourth(0, s) - own_unit[:, at] * mean) / scale[:, 0:1]
        res_all[block(0, False), cut_columns(a, s)] = residual.astype(bf16)
        residual_out[:, at] = residual
        spread(RES + s, res_all)
        for k in range(s, local_experts, 2):
            factors(k)
    for s in range(2):
        for m in range(1, n_o):
            forward(RES + s, res_all, m)
    for s in range(2):
        for m in range(n_o):
            crossed(RES + s, res_all, m)
    from_sibling(RES, res_all)
    act_terms(0, c)
    act_terms(1, c)
    act_terms(0, 1 - c)
    from_sibling(RES + 1, res_all)
    act_terms(1, 1 - c)
    for k in range(local_experts):
        hidden_grads(k)
        start(grads_copy(k))
    for d in range(n_a):
        for s in range(2):
            own_terms(1, d, s)
    for copy in pair_copies:
        copy.wait_recv()
    for k in range(local_experts):
        grads_copy(k).wait_recv()
    terms_and_first(1)
    sums = second(1)
    third(1, *sums)
    for s in range(2):
        input_out[:, s * cut:(s + 1) * cut] = fourth(1, s)
    for copy in sends:
        copy.wait_send()


def step(layer_out, moe_input, gain, head_weight, clean, levels, table, gates, ids, w_gate, w_up,
         w_down):
    n_e, n_v = lax.axis_size("expert"), lax.axis_size("vocab")
    n_o, n_a = n_e // PAIR, n_v // CORES
    rows, width = layer_out.shape
    total_rows, share = rows * n_e, width // n_v
    vocab_local = head_weight.shape[1]
    local_experts, _, hidden = w_gate.shape
    lanes = -(-(local_experts * n_e + 2) // 128) * 128
    cut = share // 2
    more = max(n_a - 1, 1)
    dma = pltpu.SemaphoreType.DMA
    small = (layer_out, gain, clean, levels, table, gates, ids)
    buffers = [pltpu.VMEM(x.shape, x.dtype) for x in small] + [
        pltpu.VMEM((total_rows, width), bf16),
        pltpu.VMEM((total_rows, width), bf16),
        pltpu.VMEM((total_rows, width), bf16),
        pltpu.VMEM((total_rows, lanes), f32),
        pltpu.VMEM((lanes, 128), f32),
        pltpu.VMEM((width, vocab_local), bf16),
        pltpu.VMEM((n_a, share, vocab_local), bf16),
        pltpu.VMEM((width, 2 * local_experts * hidden), bf16),
        pltpu.VMEM((local_experts * hidden, width), bf16),
        pltpu.VMEM((total_rows, local_experts * hidden), f32),
        pltpu.VMEM((n_a, share, 2 * local_experts * hidden), bf16),
        pltpu.VMEM((total_rows, vocab_local), bf16),
        pltpu.VMEM((total_rows, vocab_local), bf16),
        pltpu.VMEM((total_rows, 2 * local_experts * hidden), bf16),
        pltpu.VMEM((total_rows, 2 * local_experts * hidden), bf16),
        pltpu.VMEM((n_a, 2, total_rows, cut), f32),
        pltpu.VMEM((local_experts, total_rows, hidden), f32),
        pltpu.VMEM((local_experts, total_rows, hidden), f32),
        pltpu.VMEM((2, more, total_rows, cut), bf16),
        pltpu.VMEM((2, more, total_rows, cut), bf16),
        pltpu.VMEM((2, n_o, rows, cut), bf16),
        pltpu.VMEM((2, n_o, rows, cut), bf16),
        pltpu.VMEM((2, more, n_o, rows, cut), bf16),
        pltpu.VMEM((2, more, n_o, rows, cut), bf16),
        pltpu.VMEM((2, n_a, n_o, rows, cut), bf16),
        pltpu.VMEM((2, n_a, n_o, rows, cut), bf16),
        pltpu.VMEM((2, 2, n_o, rows, cut), f32),
        pltpu.VMEM((2, 2, n_o, rows, cut), f32),
        pltpu.VMEM((2, rows, cut), f32),
        pltpu.VMEM((total_rows, 128), f32),
        pltpu.VMEM((4, 8, total_rows), f32),
        pltpu.VMEM((2, 8, total_rows), f32),
        pltpu.VMEM((more, 8, total_rows), f32),
        pltpu.VMEM((n_o, 8, total_rows), f32),
        pltpu.VMEM((rows, 128), f32),
        pltpu.VMEM((rows, width), f32),
    ]
    outs = [
        pltpu.VMEM((width, total_rows), bf16),
        pltpu.VMEM((total_rows, vocab_local), bf16),
        pltpu.VMEM((rows, share), f32),
        pltpu.VMEM((rows, share), f32),
    ]
    grant = VMEM_BYTES - sum(math.prod(x.shape) * jnp.dtype(x.dtype).itemsize for x in outs)
    scratch = buffers + [
        dma((KINDS, n_o)), dma((KINDS, n_o)),
        dma((KINDS, n_o)), dma((KINDS, n_o)),
        dma((KINDS, 2 * n_o, n_a)), dma((KINDS, 2 * n_o, n_a)),
        dma((KINDS, 2 * n_o, n_a)), dma((KINDS, 2 * n_o, n_a)),
        dma((1,)), dma((1,)),
        dma((2, max(n_a, local_experts))), dma((2, max(n_a, local_experts))),
        dma((n_a, 2 * local_experts)), dma((n_a, 2 * local_experts)),
        dma((2, n_a)), dma((2, n_a)),
        dma((2,)), dma((2,)),
        dma((2, n_a)), dma((2, n_a)),
        dma((2,)), dma((2,)),
        dma((2, 2, n_o)), dma((2, 2, n_o)),
        dma((4, max(n_a, n_o))), dma((4, max(n_a, n_o))),
        dma((12 + 3 * local_experts,)),
    ]
    return pl.pallas_call(
        step_kernel,
        out_shape=outs,
        in_specs=[HBM] * 12,
        out_specs=[VMEM] * 4,
        scratch_shapes=scratch,
        compiler_params=pltpu.CompilerParams(
            collective_id=0, has_side_effects=True, vmem_limit_bytes=grant,
        ),
    )(layer_out, moe_input, gain, head_weight, clean, levels, table, gates, ids, w_gate, w_up,
      w_down)


def last_kernel(normed_ref, sg_ref, residual_ref, input_ref, head_grad, residual_out, input_out,
                tiles, sems):
    copies = [
        pltpu.make_async_copy(residual_ref, residual_out, sems.at[tiles.shape[0]]),
        pltpu.make_async_copy(input_ref, input_out, sems.at[tiles.shape[0] + 1]),
    ]
    for copy in copies:
        copy.start()
    tile = tiles.shape[1]
    for n in range(tiles.shape[0]):
        at = pl.ds(n * tile, tile)
        tiles[n] = jnp.dot(normed_ref[at, :], sg_ref[...], preferred_element_type=f32)
        copy = pltpu.make_async_copy(tiles.at[n], head_grad.at[at, :], sems.at[n])
        copy.start()
        copies.append(copy)
    for copy in copies:
        copy.wait()


def last(normed, sg, residual, input_grad):
    width = normed.shape[0]
    vocab_local = sg.shape[1]
    tiles = width // TILE
    return pl.pallas_call(
        last_kernel,
        out_shape=[
            jax.ShapeDtypeStruct((width, vocab_local), f32),
            jax.ShapeDtypeStruct(residual.shape, f32),
            jax.ShapeDtypeStruct(input_grad.shape, f32),
        ],
        in_specs=[VMEM] * 4,
        out_specs=[ANY] * 3,
        scratch_shapes=[
            pltpu.VMEM((tiles, TILE, vocab_local), f32),
            pltpu.SemaphoreType.DMA((tiles + 2,)),
        ],
        compiler_params=pltpu.CompilerParams(vmem_limit_bytes=4 * width * vocab_local + SPARE),
    )(*(pltpu.with_memory_space_constraint(x, pltpu.VMEM)
        for x in (normed, sg, residual, input_grad)))


def on_device(
    layer_out,
    moe_input,
    final_gain,
    head_weight,
    clean_ids,
    levels,
    ratio_table,
    gate_weights,
    expert_ids,
    w_gate,
    w_up,
    w_down,
):
    normed_all, score_grad, residual_grad, input_grad = step(
        layer_out, moe_input, final_gain[None, :], head_weight, clean_ids[None, :],
        levels[None, :], ratio_table[None, :], gate_weights.T, expert_ids.T, w_gate, w_up, w_down,
    )
    return tuple(last(normed_all, score_grad, residual_grad, input_grad))


def solution(mesh):
    in_specs = (
        P("expert", None),
        P("expert", None),
        P(),
        P(None, ("expert", "vocab")),
        P("expert"),
        P("expert"),
        P(),
        P("expert", None),
        P("expert", None),
        P("expert", None, "vocab"),
        P("expert", None, "vocab"),
        P("expert", "vocab", None),
    )
    out_specs = (P(None, ("expert", "vocab")), P("expert", "vocab"), P("expert", "vocab"))
    return jax.shard_map(
        on_device, mesh=mesh, in_specs=in_specs, out_specs=out_specs, check_vma=False
    )
```

```python
import functools
import math

import jax
import jax.numpy as jnp
from jax import lax
from jax.experimental import pallas as pl
from jax.experimental.pallas import tpu as pltpu
from jax.sharding import PartitionSpec as P

epsilon = 1e-05
CORES = 2
PAIR = 2
TILE = 256
SPARE = 6 << 20
VMEM_BYTES = 67043328
MESH = pl.DeviceIdType.MESH
ANY = pl.BlockSpec(memory_space=pl.ANY)
VMEM = pl.BlockSpec(memory_space=pltpu.VMEM)
HBM = pl.BlockSpec(memory_space=pltpu.HBM)
f32, bf16 = jnp.float32, jnp.bfloat16
TRANSPOSED = (((1,), (1,)), ((), ()))
NORMED, MOE, RES = range(3)
KINDS = 4
X0, Y0, X1, Y1, Z = range(5)
SG, HEAD, WEIGHTS, GRADS = range(4)


def flip(x, mask):
    bit = 1
    while bit <= mask:
        if mask & bit:
            x = x + bit - 2 * bit * ((x // bit) % 2)
        bit *= 2
    return x


def remote(src, dst, send, recv, target):
    return pltpu.make_async_remote_copy(
        src_ref=src, dst_ref=dst, send_sem=send, recv_sem=recv, device_id=target,
        device_id_type=MESH,
    )


def step_kernel(
    layer_hbm, moe_hbm, gain_hbm, head_hbm, clean_hbm, level_hbm, table_hbm, gates_hbm, ids_hbm,
    gate_hbm, up_hbm, down_hbm,
    normed_out, sg_out, residual_out, input_out,
    layer, gain, clean_ids, levels, table, gates, ids,
    normed_all, moe_all, res_all, meta_all, meta_t, head, head_pair, w_both, w_down, act,
    pair_both, sg, sg_pair, grads, grads_pair, part, fac_gate, fac_up,
    xs0, xr0, ys0, yr0, xs1, xr1, ys1, yr1, z_send, z_recv, own, dot_wide, dot_send, dot_recv, dot_chip, dot_outer, scale, unit,
    z_rs, plane_rs, sib_rs, out_ss, meta_z, meta_y, meta_one, one_ss, one_rs, rs_s, rs_r, dot_s,
    dot_r, local_sem,
):
    e, v = lax.axis_index("expert"), lax.axis_index("vocab")
    n_e, n_v = lax.axis_size("expert"), lax.axis_size("vocab")
    a, c, n_a = v // CORES, v % CORES, n_v // CORES
    o, i, n_o = e // PAIR, e % PAIR, n_e // PAIR
    rows, width = layer.shape
    total_rows = rows * n_e
    vocab_local = head_hbm.shape[1]
    local_experts, _, hidden = gate_hbm.shape
    experts_all = local_experts * n_e
    share = width // n_v
    cut = share // 2
    row_step = math.gcd(total_rows, 256)
    row_parts = [pl.ds(r, row_step) for r in range(0, total_rows, row_step)]

    def device(o_at, i_at, a_at):
        return (o_at * PAIR + i_at, a_at * CORES + c)

    sibling = (e, a * CORES + 1 - c)
    outer_peer = [device(flip(o, m), i, a) for m in range(n_o)]
    inner_peer = device(o, 1 - i, a)
    chip_at = [lax.rem(a + d, n_a) for d in range(n_a)]
    chip_from = [lax.rem(a + n_a - d, n_a) for d in range(n_a)]
    chip_peer = [device(o, i, chip_at[d]) for d in range(n_a)]
    diagonal_peer = [device(o, 1 - i, chip_at[d]) for d in range(n_a)]

    barrier = pltpu.get_barrier_semaphore()
    others = outer_peer[1:] + [inner_peer] + chip_peer[1:] + diagonal_peer[1:] + [sibling]
    for other in others:
        pl.semaphore_signal(barrier, inc=1, device_id=other, device_id_type=MESH)

    def block(m, across):
        at = flip(o, m) * PAIR + (1 - i if across else i)
        return pl.ds(pl.multiple_of(at * rows, rows), rows)

    def columns_of(at, core):
        return pl.ds(pl.multiple_of((at * CORES + core) * share, share), share)

    def cut_columns(at, s):
        return pl.ds(pl.multiple_of((at * CORES + c) * share + s * cut, cut), cut)

    def landed(ref, recv):
        remote(ref, ref, recv, recv, sibling).wait_recv()

    def left(ref, send):
        remote(ref, ref, send, send, sibling).wait_send()

    def piece(kind, buf, m, across, at, core):
        if kind >= RES:
            first = (at * CORES + core) * share + (kind - RES) * cut
            return buf.at[block(m, across), pl.ds(pl.multiple_of(first, cut), cut)]
        return buf.at[block(m, across), columns_of(at, core)]

    def post(kind, ref, recv, target, outer=False):
        remote(ref, ref, out_ss.at[kind, int(outer and kind >= RES)], recv, target).start()

    def plane(kind, buf, m):
        ref = piece(kind, buf, m, False, a, c)
        for d in range(1, n_a):
            post(kind, ref, plane_rs.at[kind, m], diagonal_peer[d])
            if m or kind >= RES:
                post(kind, ref, plane_rs.at[kind, m], chip_peer[d])
        post(kind, ref, plane_rs.at[kind, m], inner_peer)

    def to_sibling(kind, buf, m, across, d):
        post(kind, piece(kind, buf, m, across, chip_from[d], c), sib_rs.at[kind], sibling)

    def spread(kind, buf):
        ref = piece(kind, buf, 0, False, a, c)
        for m in range(1, n_o):
            post(kind, ref, z_rs.at[kind, m - 1], outer_peer[m], True)
        plane(kind, buf, 0)
        if kind >= RES:
            to_sibling(kind, buf, 0, False, 0)

    def forward(kind, buf, m):
        landed(piece(kind, buf, m, False, a, c), z_rs.at[kind, m - 1])
        plane(kind, buf, m)
        to_sibling(kind, buf, m, False, 0)

    def area(kind, buf, height, pieces):
        return buf.at[pl.ds(0, height * rows), pl.ds(0, pieces * (cut if kind >= RES else share))]

    def crossed(kind, buf, m):
        both = m > 0 or kind >= RES
        landed(area(kind, buf, 1, 2 * n_a - 1 if both else n_a), plane_rs.at[kind, m])
        to_sibling(kind, buf, m, True, 0)
        for across in ((False, True) if both else (True,)):
            for d in range(1, n_a):
                to_sibling(kind, buf, m, across, d)

    def from_sibling(kind, buf):
        landed(area(kind, buf, 2 * n_o if kind >= RES else 2 * n_o - 1, n_a), sib_rs.at[kind])

    def sent(kind, buf):
        if kind >= RES:
            left(area(kind, buf, n_o, 4 * n_a - 1), out_ss.at[kind, 0])
            left(area(kind, buf, n_o - 1, 1), out_ss.at[kind, 1])
        else:
            left(area(kind, buf, 2 * n_o - 1, 2 * n_a), out_ss.at[kind, 0])

    def lanes_of(k, j, n=1):
        return pl.ds((2 * k + j) * hidden, n * hidden)

    loads = [
        pltpu.make_async_copy(src, dst, local_sem.at[k])
        for k, (src, dst) in enumerate((
            (layer_hbm, layer), (gain_hbm, gain), (clean_hbm, clean_ids), (level_hbm, levels),
            (table_hbm, table), (gates_hbm, gates), (ids_hbm, ids), (head_hbm, head),
            (moe_hbm, moe_all.at[block(0, False)])))
    ]
    for copy in loads:
        copy.start()
    for k in range(local_experts):
        pltpu.make_async_copy(down_hbm.at[k], w_down.at[pl.ds(k * hidden, hidden), :],
                              local_sem.at[9]).start()
        for j, src in enumerate((gate_hbm, up_hbm)):
            pltpu.make_async_copy(src.at[k], w_both.at[:, lanes_of(k, j)], local_sem.at[10]).start()
    meta_t[...] = jnp.zeros_like(meta_t)
    for copy in loads[:7]:
        copy.wait()
    values = layer[...].astype(f32)
    row_scale = jnp.sqrt(jnp.sum(values * values, axis=1, keepdims=True) / width + epsilon)
    unit_rows = values / row_scale
    normed_all[block(0, False), :] = (unit_rows * gain[...]).astype(bf16)
    unit[...] = unit_rows
    scale[...] = jnp.broadcast_to(row_scale, scale.shape)
    label = lax.broadcasted_iota(jnp.int32, (experts_all, rows), 0)
    expert_gates = jnp.zeros((experts_all, rows), f32)
    for k in range(ids.shape[0]):
        expert_gates = expert_gates + jnp.where(ids[k:k + 1, :] == label, gates[k:k + 1, :], 0.0)
    ratio_row = jnp.zeros((1, rows), f32)
    for k in range(table.shape[1]):
        ratio_row = ratio_row + jnp.where(levels[...] == k, table[:, k:k + 1], 0.0)
    meta_t[0:experts_all, 0:rows] = expert_gates
    meta_t[experts_all:experts_all + 1, 0:rows] = ratio_row
    meta_t[experts_all + 1:experts_all + 2, 0:rows] = clean_ids[...].astype(f32)
    meta_all[block(0, False), :] = jnp.transpose(meta_t[...])[0:rows, :]
    pl.semaphore_wait(barrier, len(others))

    def meta_post(m, across, send, recv, target):
        ref = meta_all.at[block(m, across)]
        remote(ref, ref, meta_one.at[send], recv, target).start()

    @pl.when(c == CORES - 1)
    def _():
        for m in range(1, n_o):
            meta_post(0, False, 0, meta_z.at[m - 1], outer_peer[m])
        meta_post(0, False, 0, meta_y.at[0], inner_peer)
    spread(NORMED, normed_all)
    for d in range(n_a):
        theirs = columns_of(chip_at[d], 1 - c)
        remote(head_hbm.at[theirs, :], head_pair.at[d], one_ss.at[HEAD], one_rs.at[HEAD],
               sibling).start()
    for d in range(n_a):
        theirs = columns_of(chip_at[d], 1 - c)
        for k in range(local_experts):
            for j, src in enumerate((gate_hbm, up_hbm)):
                remote(src.at[k, theirs, :], pair_both.at[d, :, lanes_of(k, j)],
                       one_ss.at[WEIGHTS], one_rs.at[WEIGHTS], sibling).start()

    def factors(k):
        lane = lax.broadcasted_iota(jnp.int32, (1, meta_all.shape[1]), 1)
        for at in row_parts:
            x = moe_all[at, :]
            gate_pre = jnp.dot(x, w_both[:, lanes_of(k, 0)], preferred_element_type=f32)
            up_pre = jnp.dot(x, w_both[:, lanes_of(k, 1)], preferred_element_type=f32)
            weight = jnp.sum(jnp.where(lane == e * local_experts + k, meta_all[at, :], 0.0),
                             axis=1, keepdims=True)
            s = jax.nn.sigmoid(gate_pre)
            fac_gate[k, at, :] = weight * (up_pre * s * (1.0 + gate_pre * (1.0 - s)))
            fac_up[k, at, :] = weight * (gate_pre * s)

    act_seen = []

    def act_terms(s, core):
        for d in range(n_a):
            first = pl.multiple_of((chip_at[d] * CORES + core) * share + s * cut, cut)
            columns = pl.ds(first, cut)
            for at in row_parts:
                term = lax.dot_general(res_all[at, columns], w_down[:, columns], TRANSPOSED,
                                       preferred_element_type=f32)
                if act_seen:
                    act[at, :] += term
                else:
                    act[at, :] = term
            act_seen.append(d)

    def hidden_grads():
        for k in range(local_experts):
            for at in row_parts:
                own_act = act[at, pl.ds(k * hidden, hidden)]
                grads[at, lanes_of(k, 0)] = (own_act * fac_gate[k, at, :]).astype(bf16)
                grads[at, lanes_of(k, 1)] = (own_act * fac_up[k, at, :]).astype(bf16)

    def own_terms(q, d, s):
        columns = cut_columns(chip_at[d], s)
        left, right = (grads, w_both) if q else (sg, head)
        for at in row_parts:
            part[d, s, at, :] = lax.dot_general(left[at, :], right[columns, :], TRANSPOSED,
                                                preferred_element_type=f32)

    def pair_terms(q, d, s):
        columns = pl.ds(s * cut, cut)
        left, right = (grads_pair, pair_both) if q else (sg_pair, head_pair)
        for at in row_parts:
            part[d, s, at, :] += lax.dot_general(left[at, :], right[d, columns, :], TRANSPOSED,
                                                 preferred_element_type=f32)

    def scores():
        for at in row_parts:
            x = normed_all[at, :]
            meta = meta_all[at, :]
            ratio = meta[:, experts_all:experts_all + 1]
            clean = meta[:, experts_all + 1:experts_all + 2]
            score = jnp.dot(x, head[...], preferred_element_type=f32)
            label = (e * n_v + v) * vocab_local + lax.broadcasted_iota(
                jnp.int32, (1, vocab_local), 1)
            hit = jnp.where(clean == label.astype(f32), ratio, 0.0)
            grad = ((jnp.exp(score) - hit) * (1.0 / math.sqrt(total_rows))).astype(bf16)
            sg[at, :] = grad
            dot = jnp.sum(grad.astype(f32) * score, axis=1, keepdims=True)
            dot_wide[at, :] = jnp.broadcast_to(dot, (row_step, 128))
        dot_send[0] = jnp.transpose(dot_wide[...])[0:8, :]

    def exchange(q, stage, src, dst, target):
        remote(src, dst, rs_s.at[q, stage], rs_r.at[q, stage], target).start()

    def terms_and_first(q):
        for d in range(1, n_a):
            pair_terms(q, d, 0)
            xs0[q, d - 1] = part[d, 0].astype(bf16)
            exchange(q, X0, xs0.at[q, d - 1], xr0.at[q, d - 1], chip_peer[d])
        for d in list(range(1, n_a)) + [0]:
            pair_terms(q, d, 1)
            for m in range(n_o):
                ys1[q, d, m] = part[d, 1, block(m, True), :].astype(bf16)
            exchange(q, Y1, ys1.at[q, d], yr1.at[q, d], inner_peer)
        own_terms(q, 0, 0)
        pair_terms(q, 0, 0)

    def dot_start(stage):
        src = dot_send.at[stage]
        if stage == 0:
            targets = [(dot_recv.at[0], sibling)]
        elif stage == 1:
            targets = [(dot_chip.at[d - 1], chip_peer[d]) for d in range(1, n_a)]
        elif stage == 2:
            targets = [(dot_recv.at[1], inner_peer)]
        else:
            targets = [(dot_outer.at[m - 1], outer_peer[m]) for m in range(1, n_o)]
        for dst, target in targets:
            remote(src, dst, dot_s.at[stage], dot_r.at[stage], target).start()

    dot_whole = [dot_recv.at[0], dot_chip, dot_recv.at[1], dot_outer]

    def dot_sum(stage):
        landed(dot_whole[stage], dot_r.at[stage])
        total = dot_send[stage]
        if stage == 0:
            return total + dot_recv[0]
        if stage == 1:
            for d in range(1, n_a):
                total = total + dot_chip[d - 1]
            return total
        if stage == 2:
            return total + dot_recv[1]
        for m in range(1, n_o):
            total = total + dot_outer[m - 1]
        return total

    def dot_next(stage):
        dot_send[stage + 1] = dot_sum(stage)
        dot_start(stage + 1)

    def second(q):
        landed(xr0.at[q], rs_r.at[q, X0])
        if q == 0:
            dot_next(1)

        def sum_0(m, across):
            at = block(m, across)
            term = part[0, 0, at, :]
            for d in range(1, n_a):
                term = term + xr0[q, d - 1, at, :].astype(f32)
            return term

        for m in range(n_o):
            ys0[q, m] = sum_0(m, True).astype(bf16)
        exchange(q, Y0, ys0.at[q], yr0.at[q], inner_peer)
        landed(yr1.at[q], rs_r.at[q, Y1])

        def sum_1(d, m):
            return part[d, 1, block(m, False), :] + yr1[q, d, m].astype(f32)

        for d in range(1, n_a):
            for m in range(n_o):
                xs1[q, d - 1, m] = sum_1(d, m).astype(bf16)
            exchange(q, X1, xs1.at[q, d - 1], xr1.at[q, d - 1], chip_peer[d])
        return sum_0, sum_1

    def z_post(q, s, m, term):
        if m:
            z_send[q, s, m - 1] = term
            exchange(q, Z + s, z_send.at[q, s, m - 1], z_recv.at[q, s, m - 1], outer_peer[m])
        else:
            own[s] = term

    def third(q, sum_0, sum_1):
        landed(yr0.at[q], rs_r.at[q, Y0])
        if q == 0:
            dot_next(2)
        for m in list(range(1, n_o)) + [0]:
            z_post(q, 0, m, sum_0(m, False) + yr0[q, m].astype(f32))
        landed(xr1.at[q], rs_r.at[q, X1])
        for m in list(range(1, n_o)) + [0]:
            term = sum_1(0, m)
            for d in range(1, n_a):
                term = term + xr1[q, d - 1, m].astype(f32)
            z_post(q, 1, m, term)

    def fourth(q, s):
        landed(z_recv.at[q, s], rs_r.at[q, Z + s])
        term = own[s]
        for m in range(1, n_o):
            term = term + z_recv[q, s, m - 1]
        return term

    for m in range(1, n_o):
        @pl.when(c == CORES - 1)
        def _():
            landed(meta_all.at[block(m, False)], meta_z.at[m - 1])
            meta_post(m, False, 0, meta_y.at[m], inner_peer)
            meta_post(m, False, 1, meta_one.at[2], sibling)
        forward(NORMED, normed_all, m)
    loads[8].wait()
    spread(MOE, moe_all)
    for m in range(n_o):
        crossed(NORMED, normed_all, m)
    meta_area = meta_all.at[pl.ds(0, (2 * n_o - 1) * rows)]

    @pl.when(c == CORES - 1)
    def _():
        for m in range(n_o):
            landed(meta_all.at[block(m, True)], meta_y.at[m])
            meta_post(m, True, 1, meta_one.at[2], sibling)
        left(meta_area, meta_one.at[0])
        left(meta_area, meta_one.at[1])
    for m in range(1, n_o):
        forward(MOE, moe_all, m)

    @pl.when(c == 0)
    def _():
        landed(meta_area, meta_one.at[2])
    loads[7].wait()
    from_sibling(NORMED, normed_all)
    scores()
    remote(sg, sg_pair, one_ss.at[SG], one_rs.at[SG], sibling).start()
    dot_start(0)
    for d in range(1, n_a):
        own_terms(0, d, 0)
    for d in range(n_a):
        own_terms(0, d, 1)
    landed(head_pair, one_rs.at[HEAD])
    landed(sg_pair, one_rs.at[SG])
    dot_next(0)
    terms_and_first(0)
    for at in row_parts:
        for n in range(0, width, row_step):
            normed_out[pl.ds(n, row_step), at] = jnp.transpose(normed_all[at, pl.ds(n, row_step)])
    sg_out[...] = sg[...]
    sums = second(0)
    pltpu.make_async_copy(w_down, w_down, local_sem.at[9]).wait()
    pltpu.make_async_copy(w_both, w_both, local_sem.at[10]).wait()
    third(0, *sums)
    for m in range(n_o):
        crossed(MOE, moe_all, m)
    from_sibling(MOE, moe_all)
    dot_total = dot_sum(3)
    dot_wide[...] = jnp.transpose(jnp.broadcast_to(dot_total[0:1, :], (128, total_rows)))
    mean = dot_wide[block(0, False), 0:1] / width
    own_gain = gain[:, columns_of(a, c)]
    own_unit = unit[:, columns_of(a, c)]
    for s in range(2):
        at = slice(s * cut, (s + 1) * cut)
        residual = (own_gain[:, at] * fourth(0, s) - own_unit[:, at] * mean) / scale[:, 0:1]
        res_all[block(0, False), cut_columns(a, s)] = residual.astype(bf16)
        residual_out[:, at] = residual
        spread(RES + s, res_all)
        for k in range(s, local_experts, 2):
            factors(k)
    for s in range(2):
        for m in range(1, n_o):
            forward(RES + s, res_all, m)
    for s in range(2):
        for m in range(n_o):
            crossed(RES + s, res_all, m)
    from_sibling(RES, res_all)
    act_terms(0, c)
    act_terms(1, c)
    act_terms(0, 1 - c)
    from_sibling(RES + 1, res_all)
    act_terms(1, 1 - c)
    hidden_grads()
    remote(grads, grads_pair, one_ss.at[GRADS], one_rs.at[GRADS], sibling).start()
    for d in range(1, n_a):
        own_terms(1, d, 0)
    for d in range(n_a):
        own_terms(1, d, 1)
    landed(pair_both, one_rs.at[WEIGHTS])
    landed(grads_pair, one_rs.at[GRADS])
    terms_and_first(1)
    sums = second(1)
    third(1, *sums)
    for s in range(2):
        input_out[:, s * cut:(s + 1) * cut] = fourth(1, s)
    sent(NORMED, normed_all)
    sent(MOE, moe_all)
    for s in range(2):
        sent(RES + s, res_all)
    left(sg, one_ss.at[SG])
    left(head_pair, one_ss.at[HEAD])
    left(pair_both, one_ss.at[WEIGHTS])
    left(grads, one_ss.at[GRADS])
    for q in range(2):
        for stage, buf in ((X0, xs0), (Y0, ys0), (X1, xs1), (Y1, ys1)):
            left(buf.at[q], rs_s.at[q, stage])
        for s in range(2):
            left(z_send.at[q, s], rs_s.at[q, Z + s])
    for stage in range(4):
        left(dot_whole[stage], dot_s.at[stage])


def step(layer_out, moe_input, gain, head_weight, clean, levels, table, gates, ids, w_gate, w_up,
         w_down):
    n_e, n_v = lax.axis_size("expert"), lax.axis_size("vocab")
    n_o, n_a = n_e // PAIR, n_v // CORES
    rows, width = layer_out.shape
    total_rows, share = rows * n_e, width // n_v
    vocab_local = head_weight.shape[1]
    local_experts, _, hidden = w_gate.shape
    lanes = -(-(local_experts * n_e + 2) // 128) * 128
    cut = share // 2
    more = max(n_a - 1, 1)
    dma = pltpu.SemaphoreType.DMA
    small = (layer_out, gain, clean, levels, table, gates, ids)
    buffers = [pltpu.VMEM(x.shape, x.dtype) for x in small] + [
        pltpu.VMEM((total_rows, width), bf16),
        pltpu.VMEM((total_rows, width), bf16),
        pltpu.VMEM((total_rows, width), bf16),
        pltpu.VMEM((total_rows, lanes), f32),
        pltpu.VMEM((lanes, 128), f32),
        pltpu.VMEM((width, vocab_local), bf16),
        pltpu.VMEM((n_a, share, vocab_local), bf16),
        pltpu.VMEM((width, 2 * local_experts * hidden), bf16),
        pltpu.VMEM((local_experts * hidden, width), bf16),
        pltpu.VMEM((total_rows, local_experts * hidden), f32),
        pltpu.VMEM((n_a, share, 2 * local_experts * hidden), bf16),
        pltpu.VMEM((total_rows, vocab_local), bf16),
        pltpu.VMEM((total_rows, vocab_local), bf16),
        pltpu.VMEM((total_rows, 2 * local_experts * hidden), bf16),
        pltpu.VMEM((total_rows, 2 * local_experts * hidden), bf16),
        pltpu.VMEM((n_a, 2, total_rows, cut), f32),
        pltpu.VMEM((local_experts, total_rows, hidden), f32),
        pltpu.VMEM((local_experts, total_rows, hidden), f32),
        pltpu.VMEM((2, more, total_rows, cut), bf16),
        pltpu.VMEM((2, more, total_rows, cut), bf16),
        pltpu.VMEM((2, n_o, rows, cut), bf16),
        pltpu.VMEM((2, n_o, rows, cut), bf16),
        pltpu.VMEM((2, more, n_o, rows, cut), bf16),
        pltpu.VMEM((2, more, n_o, rows, cut), bf16),
        pltpu.VMEM((2, n_a, n_o, rows, cut), bf16),
        pltpu.VMEM((2, n_a, n_o, rows, cut), bf16),
        pltpu.VMEM((2, 2, n_o - 1, rows, cut), f32),
        pltpu.VMEM((2, 2, n_o - 1, rows, cut), f32),
        pltpu.VMEM((2, rows, cut), f32),
        pltpu.VMEM((total_rows, 128), f32),
        pltpu.VMEM((4, 8, total_rows), f32),
        pltpu.VMEM((2, 8, total_rows), f32),
        pltpu.VMEM((more, 8, total_rows), f32),
        pltpu.VMEM((n_o - 1, 8, total_rows), f32),
        pltpu.VMEM((rows, 128), f32),
        pltpu.VMEM((rows, width), f32),
    ]
    outs = [
        pltpu.VMEM((width, total_rows), bf16),
        pltpu.VMEM((total_rows, vocab_local), bf16),
        pltpu.VMEM((rows, share), f32),
        pltpu.VMEM((rows, share), f32),
    ]
    grant = VMEM_BYTES - sum(math.prod(x.shape) * jnp.dtype(x.dtype).itemsize for x in outs)
    scratch = buffers + [
        dma((KINDS, n_o - 1)), dma((KINDS, n_o)), dma((KINDS,)), dma((KINDS, 2)),
        dma((n_o - 1,)), dma((n_o,)), dma((3,)),
        dma((4,)), dma((4,)),
        dma((2, 6)), dma((2, 6)),
        dma((4,)), dma((4,)),
        dma((11,)),
    ]
    return pl.pallas_call(
        step_kernel,
        out_shape=outs,
        in_specs=[HBM] * 12,
        out_specs=[VMEM] * 4,
        scratch_shapes=scratch,
        compiler_params=pltpu.CompilerParams(
            collective_id=0, has_side_effects=True, vmem_limit_bytes=grant,
        ),
    )(layer_out, moe_input, gain, head_weight, clean, levels, table, gates, ids, w_gate, w_up,
      w_down)


def last_kernel(normed_ref, sg_ref, residual_ref, input_ref, head_grad, residual_out, input_out,
                tiles, sems):
    copies = [
        pltpu.make_async_copy(residual_ref, residual_out, sems.at[tiles.shape[0]]),
        pltpu.make_async_copy(input_ref, input_out, sems.at[tiles.shape[0] + 1]),
    ]
    for copy in copies:
        copy.start()
    tile = tiles.shape[1]
    for n in range(tiles.shape[0]):
        at = pl.ds(n * tile, tile)
        tiles[n] = jnp.dot(normed_ref[at, :], sg_ref[...], preferred_element_type=f32)
        copy = pltpu.make_async_copy(tiles.at[n], head_grad.at[at, :], sems.at[n])
        copy.start()
        copies.append(copy)
    for copy in copies:
        copy.wait()


def last(normed, sg, residual, input_grad):
    width = normed.shape[0]
    vocab_local = sg.shape[1]
    tiles = width // TILE
    return pl.pallas_call(
        last_kernel,
        out_shape=[
            jax.ShapeDtypeStruct((width, vocab_local), f32),
            jax.ShapeDtypeStruct(residual.shape, f32),
            jax.ShapeDtypeStruct(input_grad.shape, f32),
        ],
        in_specs=[VMEM] * 4,
        out_specs=[ANY] * 3,
        scratch_shapes=[
            pltpu.VMEM((tiles, TILE, vocab_local), f32),
            pltpu.SemaphoreType.DMA((tiles + 2,)),
        ],
        compiler_params=pltpu.CompilerParams(vmem_limit_bytes=4 * width * vocab_local + SPARE),
    )(*(pltpu.with_memory_space_constraint(x, pltpu.VMEM)
        for x in (normed, sg, residual, input_grad)))


def on_device(
    layer_out,
    moe_input,
    final_gain,
    head_weight,
    clean_ids,
    levels,
    ratio_table,
    gate_weights,
    expert_ids,
    w_gate,
    w_up,
    w_down,
):
    normed_all, score_grad, residual_grad, input_grad = step(
        layer_out, moe_input, final_gain[None, :], head_weight, clean_ids[None, :],
        levels[None, :], ratio_table[None, :], gate_weights.T, expert_ids.T, w_gate, w_up, w_down,
    )
    return tuple(last(normed_all, score_grad, residual_grad, input_grad))


def solution(mesh):
    in_specs = (
        P("expert", None),
        P("expert", None),
        P(),
        P(None, ("expert", "vocab")),
        P("expert"),
        P("expert"),
        P(),
        P("expert", None),
        P("expert", None),
        P("expert", None, "vocab"),
        P("expert", None, "vocab"),
        P("expert", "vocab", None),
    )
    out_specs = (P(None, ("expert", "vocab")), P("expert", "vocab"), P("expert", "vocab"))
    return jax.shard_map(
        on_device, mesh=mesh, in_specs=in_specs, out_specs=out_specs, check_vma=False
    )
```

```python
import functools
import math

import jax
import jax.numpy as jnp
from jax import lax
from jax.experimental import pallas as pl
from jax.experimental.pallas import tpu as pltpu
from jax.sharding import PartitionSpec as P

epsilon = 1e-05
CORES = 2
PAIR = 2
TILE = 256
SPARE = 6 << 20
VMEM_BYTES = 67043328
MESH = pl.DeviceIdType.MESH
ANY = pl.BlockSpec(memory_space=pl.ANY)
VMEM = pl.BlockSpec(memory_space=pltpu.VMEM)
HBM = pl.BlockSpec(memory_space=pltpu.HBM)
f32, bf16 = jnp.float32, jnp.bfloat16
TRANSPOSED = (((1,), (1,)), ((), ()))
NORMED, MOE, RES = range(3)
KINDS = 4
SG, HEAD, WEIGHTS, GRADS = range(4)


def flip(x, mask):
    bit = 1
    while bit <= mask:
        if mask & bit:
            x = x + bit - 2 * bit * ((x // bit) % 2)
        bit *= 2
    return x


def remote(src, dst, send, recv, target):
    return pltpu.make_async_remote_copy(
        src_ref=src, dst_ref=dst, send_sem=send, recv_sem=recv, device_id=target,
        device_id_type=MESH,
    )


def step_kernel(
    layer_hbm, moe_hbm, gain_hbm, head_hbm, clean_hbm, level_hbm, table_hbm, gates_hbm, ids_hbm,
    gate_hbm, up_hbm, down_hbm,
    normed_out, sg_out, residual_out, input_out,
    layer, gain, clean_ids, levels, table, gates, ids,
    normed_all, moe_all, res_all, meta_all, meta_t, head, head_pair, w_both, w_down, act,
    pair_both, sg, sg_pair, grads, grads_pair, part, fac_gate, fac_up,
    p_send, p_recv, z_send_0, z_recv_0, z_send_1, z_recv_1, own, dot_wide, dot_send, dot_recv, dot_chip, dot_outer, scale, unit,
    z_rs, plane_rs, sib_rs, out_ss, meta_z, meta_y, meta_one, one_ss, one_rs, rs_s, rs_r, dot_s,
    dot_r, local_sem,
):
    e, v = lax.axis_index("expert"), lax.axis_index("vocab")
    n_e, n_v = lax.axis_size("expert"), lax.axis_size("vocab")
    a, c, n_a = v // CORES, v % CORES, n_v // CORES
    o, i, n_o = e // PAIR, e % PAIR, n_e // PAIR
    rows, width = layer.shape
    total_rows = rows * n_e
    vocab_local = head_hbm.shape[1]
    local_experts, _, hidden = gate_hbm.shape
    experts_all = local_experts * n_e
    share = width // n_v
    cut = share // 2
    row_step = math.gcd(total_rows, 256)
    row_parts = [pl.ds(r, row_step) for r in range(0, total_rows, row_step)]

    def device(o_at, i_at, a_at):
        return (o_at * PAIR + i_at, a_at * CORES + c)

    sibling = (e, a * CORES + 1 - c)
    outer_peer = [device(flip(o, m), i, a) for m in range(n_o)]
    inner_peer = device(o, 1 - i, a)
    chip_at = [lax.rem(a + d, n_a) for d in range(n_a)]
    chip_from = [lax.rem(a + n_a - d, n_a) for d in range(n_a)]
    chip_peer = [device(o, i, chip_at[d]) for d in range(n_a)]
    diagonal_peer = [device(o, 1 - i, chip_at[d]) for d in range(n_a)]

    barrier = pltpu.get_barrier_semaphore()
    others = outer_peer[1:] + [inner_peer] + chip_peer[1:] + diagonal_peer[1:] + [sibling]
    for other in others:
        pl.semaphore_signal(barrier, inc=1, device_id=other, device_id_type=MESH)

    def block(m, across):
        at = flip(o, m) * PAIR + (1 - i if across else i)
        return pl.ds(pl.multiple_of(at * rows, rows), rows)

    def columns_of(at, core):
        return pl.ds(pl.multiple_of((at * CORES + core) * share, share), share)

    def cut_columns(at, s):
        return pl.ds(pl.multiple_of((at * CORES + c) * share + s * cut, cut), cut)

    def landed(ref, recv):
        remote(ref, ref, recv, recv, sibling).wait_recv()

    def left(ref, send):
        remote(ref, ref, send, send, sibling).wait_send()

    def piece(kind, buf, m, across, at, core):
        if kind >= RES:
            first = (at * CORES + core) * share + (kind - RES) * cut
            return buf.at[block(m, across), pl.ds(pl.multiple_of(first, cut), cut)]
        return buf.at[block(m, across), columns_of(at, core)]

    def post(kind, ref, recv, target, outer=False):
        remote(ref, ref, out_ss.at[kind, int(outer and kind >= RES)], recv, target).start()

    def plane(kind, buf, m):
        ref = piece(kind, buf, m, False, a, c)
        for d in range(1, n_a):
            post(kind, ref, plane_rs.at[kind, m], diagonal_peer[d])
            if m or kind >= RES:
                post(kind, ref, plane_rs.at[kind, m], chip_peer[d])
        post(kind, ref, plane_rs.at[kind, m], inner_peer)

    def to_sibling(kind, buf, m, across, d):
        post(kind, piece(kind, buf, m, across, chip_from[d], c), sib_rs.at[kind], sibling)

    def spread(kind, buf):
        ref = piece(kind, buf, 0, False, a, c)
        for m in range(1, n_o):
            post(kind, ref, z_rs.at[kind, m - 1], outer_peer[m], True)
        plane(kind, buf, 0)
        if kind >= RES:
            to_sibling(kind, buf, 0, False, 0)

    def forward(kind, buf, m):
        landed(piece(kind, buf, m, False, a, c), z_rs.at[kind, m - 1])
        plane(kind, buf, m)
        to_sibling(kind, buf, m, False, 0)

    def area(kind, buf, height, pieces):
        return buf.at[pl.ds(0, height * rows), pl.ds(0, pieces * (cut if kind >= RES else share))]

    def crossed(kind, buf, m):
        both = m > 0 or kind >= RES
        landed(area(kind, buf, 1, 2 * n_a - 1 if both else n_a), plane_rs.at[kind, m])
        to_sibling(kind, buf, m, True, 0)
        for across in ((False, True) if both else (True,)):
            for d in range(1, n_a):
                to_sibling(kind, buf, m, across, d)

    def from_sibling(kind, buf):
        landed(area(kind, buf, 2 * n_o if kind >= RES else 2 * n_o - 1, n_a), sib_rs.at[kind])

    def sent(kind, buf):
        if kind >= RES:
            left(area(kind, buf, n_o, 4 * n_a - 1), out_ss.at[kind, 0])
            left(area(kind, buf, n_o - 1, 1), out_ss.at[kind, 1])
        else:
            left(area(kind, buf, 2 * n_o - 1, 2 * n_a), out_ss.at[kind, 0])

    def lanes_of(k, j, n=1):
        return pl.ds((2 * k + j) * hidden, n * hidden)

    loads = [
        pltpu.make_async_copy(src, dst, local_sem.at[k])
        for k, (src, dst) in enumerate((
            (layer_hbm, layer), (gain_hbm, gain), (clean_hbm, clean_ids), (level_hbm, levels),
            (table_hbm, table), (gates_hbm, gates), (ids_hbm, ids), (head_hbm, head),
            (moe_hbm, moe_all.at[block(0, False)])))
    ]
    for copy in loads:
        copy.start()
    for k in range(local_experts):
        pltpu.make_async_copy(down_hbm.at[k], w_down.at[pl.ds(k * hidden, hidden), :],
                              local_sem.at[9]).start()
        for j, src in enumerate((gate_hbm, up_hbm)):
            pltpu.make_async_copy(src.at[k], w_both.at[:, lanes_of(k, j)], local_sem.at[10]).start()
    meta_t[...] = jnp.zeros_like(meta_t)
    for copy in loads[:7]:
        copy.wait()
    values = layer[...].astype(f32)
    row_scale = jnp.sqrt(jnp.sum(values * values, axis=1, keepdims=True) / width + epsilon)
    unit_rows = values / row_scale
    normed_all[block(0, False), :] = (unit_rows * gain[...]).astype(bf16)
    unit[...] = unit_rows
    scale[...] = jnp.broadcast_to(row_scale, scale.shape)
    label = lax.broadcasted_iota(jnp.int32, (experts_all, rows), 0)
    expert_gates = jnp.zeros((experts_all, rows), f32)
    for k in range(ids.shape[0]):
        expert_gates = expert_gates + jnp.where(ids[k:k + 1, :] == label, gates[k:k + 1, :], 0.0)
    ratio_row = jnp.zeros((1, rows), f32)
    for k in range(table.shape[1]):
        ratio_row = ratio_row + jnp.where(levels[...] == k, table[:, k:k + 1], 0.0)
    meta_t[0:experts_all, 0:rows] = expert_gates
    meta_t[experts_all:experts_all + 1, 0:rows] = ratio_row
    meta_t[experts_all + 1:experts_all + 2, 0:rows] = clean_ids[...].astype(f32)
    meta_all[block(0, False), :] = jnp.transpose(meta_t[...])[0:rows, :]
    pl.semaphore_wait(barrier, len(others))

    def meta_post(m, across, send, recv, target):
        ref = meta_all.at[block(m, across)]
        remote(ref, ref, meta_one.at[send], recv, target).start()

    @pl.when(c == CORES - 1)
    def _():
        for m in range(1, n_o):
            meta_post(0, False, 0, meta_z.at[m - 1], outer_peer[m])
        meta_post(0, False, 0, meta_y.at[0], inner_peer)
    spread(NORMED, normed_all)
    for d in range(n_a):
        theirs = columns_of(chip_at[d], 1 - c)
        remote(head_hbm.at[theirs, :], head_pair.at[d], one_ss.at[HEAD], one_rs.at[HEAD],
               sibling).start()
    for d in range(n_a):
        theirs = columns_of(chip_at[d], 1 - c)
        for k in range(local_experts):
            for j, src in enumerate((gate_hbm, up_hbm)):
                remote(src.at[k, theirs, :], pair_both.at[d, :, lanes_of(k, j)],
                       one_ss.at[WEIGHTS], one_rs.at[WEIGHTS], sibling).start()

    def factors(k):
        lane = lax.broadcasted_iota(jnp.int32, (1, meta_all.shape[1]), 1)
        for at in row_parts:
            x = moe_all[at, :]
            gate_pre = jnp.dot(x, w_both[:, lanes_of(k, 0)], preferred_element_type=f32)
            up_pre = jnp.dot(x, w_both[:, lanes_of(k, 1)], preferred_element_type=f32)
            weight = jnp.sum(jnp.where(lane == e * local_experts + k, meta_all[at, :], 0.0),
                             axis=1, keepdims=True)
            s = jax.nn.sigmoid(gate_pre)
            fac_gate[k, at, :] = weight * (up_pre * s * (1.0 + gate_pre * (1.0 - s)))
            fac_up[k, at, :] = weight * (gate_pre * s)

    act_seen = []

    def act_terms(s, core):
        for d in range(n_a):
            first = pl.multiple_of((chip_at[d] * CORES + core) * share + s * cut, cut)
            columns = pl.ds(first, cut)
            for at in row_parts:
                term = lax.dot_general(res_all[at, columns], w_down[:, columns], TRANSPOSED,
                                       preferred_element_type=f32)
                if act_seen:
                    act[at, :] += term
                else:
                    act[at, :] = term
            act_seen.append(d)

    def hidden_grads():
        for k in range(local_experts):
            for at in row_parts:
                own_act = act[at, pl.ds(k * hidden, hidden)]
                grads[at, lanes_of(k, 0)] = (own_act * fac_gate[k, at, :]).astype(bf16)
                grads[at, lanes_of(k, 1)] = (own_act * fac_up[k, at, :]).astype(bf16)

    def own_terms(q, d, s):
        columns = cut_columns(chip_at[d], s)
        left, right = (grads, w_both) if q else (sg, head)
        for at in row_parts:
            part[d, s, at, :] = lax.dot_general(left[at, :], right[columns, :], TRANSPOSED,
                                                preferred_element_type=f32)

    def pair_terms(q, d, s):
        columns = pl.ds(s * cut, cut)
        left, right = (grads_pair, pair_both) if q else (sg_pair, head_pair)
        for at in row_parts:
            part[d, s, at, :] += lax.dot_general(left[at, :], right[d, columns, :], TRANSPOSED,
                                                 preferred_element_type=f32)

    def scores():
        for at in row_parts:
            x = normed_all[at, :]
            meta = meta_all[at, :]
            ratio = meta[:, experts_all:experts_all + 1]
            clean = meta[:, experts_all + 1:experts_all + 2]
            score = jnp.dot(x, head[...], preferred_element_type=f32)
            label = (e * n_v + v) * vocab_local + lax.broadcasted_iota(
                jnp.int32, (1, vocab_local), 1)
            hit = jnp.where(clean == label.astype(f32), ratio, 0.0)
            grad = ((jnp.exp(score) - hit) * (1.0 / math.sqrt(total_rows))).astype(bf16)
            sg[at, :] = grad
            dot = jnp.sum(grad.astype(f32) * score, axis=1, keepdims=True)
            dot_wide[at, :] = jnp.broadcast_to(dot, (row_step, 128))
        dot_send[0] = jnp.transpose(dot_wide[...])[0:8, :]

    def exchange(q, stage, src, dst, target):
        remote(src, dst, rs_s.at[q, stage], rs_r.at[q, stage], target).start()

    z_send, z_recv = (z_send_0, z_send_1), (z_recv_0, z_recv_1)
    corners = [(d, across) for d in range(n_a) for across in (False, True) if d or across]
    corner_peer = [device(o, 1 - i if across else i, chip_at[d]) for d, across in corners]

    def terms_and_first(q):
        for s in range(2):
            for d in list(range(1, n_a)) + [0]:
                pair_terms(q, d, s)
                for j, (to, across) in enumerate(corners):
                    if to == d:
                        for m in range(n_o):
                            p_send[q, s, j, m] = part[d, s, block(m, across), :].astype(bf16)
                        exchange(q, s, p_send.at[q, s, j], p_recv.at[q, s, j], corner_peer[j])

    def dot_start(stage):
        src = dot_send.at[stage]
        if stage == 0:
            targets = [(dot_recv, sibling)]
        elif stage == 1:
            targets = [(dot_chip.at[j], peer) for j, peer in enumerate(corner_peer)]
        else:
            targets = [(dot_outer.at[m - 1], outer_peer[m]) for m in range(1, n_o)]
        for dst, target in targets:
            remote(src, dst, dot_s.at[stage], dot_r.at[stage], target).start()

    dot_whole = [dot_recv, dot_chip, dot_outer]

    def dot_sum(stage):
        landed(dot_whole[stage], dot_r.at[stage])
        total = dot_send[stage]
        if stage == 0:
            return total + dot_recv[...]
        for j in range(dot_whole[stage].shape[0]):
            total = total + dot_whole[stage][j]
        return total

    def dot_next(stage):
        dot_send[stage + 1] = dot_sum(stage)
        dot_start(stage + 1)

    def third(q):
        for s in range(2):
            landed(p_recv.at[q, s], rs_r.at[q, s])
            if q == 0 and s == 0:
                dot_next(1)
            for m in list(range(2, n_o)) + [1, 0]:
                term = part[0, s, block(m, False), :]
                for j in range(len(corners)):
                    term = term + p_recv[q, s, j, m].astype(f32)
                if m:
                    z_send[q][s, m - 1] = term.astype(z_send[q].dtype)
                    exchange(q, 2 + s, z_send[q].at[s, m - 1], z_recv[q].at[s, m - 1],
                             outer_peer[m])
                else:
                    own[s] = term

    def fourth(q, s):
        landed(z_recv[q].at[s], rs_r.at[q, 2 + s])
        term = own[s]
        for m in range(1, n_o):
            term = term + z_recv[q][s, m - 1].astype(f32)
        return term

    for m in range(1, n_o):
        @pl.when(c == CORES - 1)
        def _():
            landed(meta_all.at[block(m, False)], meta_z.at[m - 1])
            meta_post(m, False, 0, meta_y.at[m], inner_peer)
            meta_post(m, False, 1, meta_one.at[2], sibling)
        forward(NORMED, normed_all, m)
    loads[8].wait()
    spread(MOE, moe_all)
    for m in range(n_o):
        crossed(NORMED, normed_all, m)
    meta_area = meta_all.at[pl.ds(0, (2 * n_o - 1) * rows)]

    @pl.when(c == CORES - 1)
    def _():
        for m in range(n_o):
            landed(meta_all.at[block(m, True)], meta_y.at[m])
            meta_post(m, True, 1, meta_one.at[2], sibling)
        left(meta_area, meta_one.at[0])
        left(meta_area, meta_one.at[1])
    for m in range(1, n_o):
        forward(MOE, moe_all, m)

    @pl.when(c == 0)
    def _():
        landed(meta_area, meta_one.at[2])
    loads[7].wait()
    from_sibling(NORMED, normed_all)
    scores()
    remote(sg, sg_pair, one_ss.at[SG], one_rs.at[SG], sibling).start()
    dot_start(0)
    for s in range(2):
        for d in list(range(1, n_a)) + [0]:
            own_terms(0, d, s)
    landed(head_pair, one_rs.at[HEAD])
    landed(sg_pair, one_rs.at[SG])
    dot_next(0)
    terms_and_first(0)
    for at in row_parts:
        for n in range(0, width, row_step):
            normed_out[pl.ds(n, row_step), at] = jnp.transpose(normed_all[at, pl.ds(n, row_step)])
    sg_out[...] = sg[...]
    pltpu.make_async_copy(w_down, w_down, local_sem.at[9]).wait()
    pltpu.make_async_copy(w_both, w_both, local_sem.at[10]).wait()
    third(0)
    for m in range(n_o):
        crossed(MOE, moe_all, m)
    from_sibling(MOE, moe_all)
    dot_total = dot_sum(2)
    dot_wide[...] = jnp.transpose(jnp.broadcast_to(dot_total[0:1, :], (128, total_rows)))
    mean = dot_wide[block(0, False), 0:1] / width
    own_gain = gain[:, columns_of(a, c)]
    own_unit = unit[:, columns_of(a, c)]
    for s in range(2):
        at = slice(s * cut, (s + 1) * cut)
        residual = (own_gain[:, at] * fourth(0, s) - own_unit[:, at] * mean) / scale[:, 0:1]
        res_all[block(0, False), cut_columns(a, s)] = residual.astype(bf16)
        residual_out[:, at] = residual
        spread(RES + s, res_all)
        for k in range(s, local_experts, 2):
            factors(k)
    for s in range(2):
        for m in range(1, n_o):
            forward(RES + s, res_all, m)
    for s in range(2):
        for m in range(n_o):
            crossed(RES + s, res_all, m)
    from_sibling(RES, res_all)
    act_terms(0, c)
    act_terms(1, c)
    act_terms(0, 1 - c)
    from_sibling(RES + 1, res_all)
    act_terms(1, 1 - c)
    hidden_grads()
    remote(grads, grads_pair, one_ss.at[GRADS], one_rs.at[GRADS], sibling).start()
    for s in range(2):
        for d in list(range(1, n_a)) + [0]:
            own_terms(1, d, s)
    landed(pair_both, one_rs.at[WEIGHTS])
    landed(grads_pair, one_rs.at[GRADS])
    terms_and_first(1)
    third(1)
    for s in range(2):
        input_out[:, s * cut:(s + 1) * cut] = fourth(1, s)
    sent(NORMED, normed_all)
    sent(MOE, moe_all)
    for s in range(2):
        sent(RES + s, res_all)
    left(sg, one_ss.at[SG])
    left(head_pair, one_ss.at[HEAD])
    left(pair_both, one_ss.at[WEIGHTS])
    left(grads, one_ss.at[GRADS])
    for q in range(2):
        for s in range(2):
            left(p_send.at[q, s], rs_s.at[q, s])
            left(z_send[q].at[s], rs_s.at[q, 2 + s])
    for stage in range(3):
        left(dot_whole[stage], dot_s.at[stage])


def step(layer_out, moe_input, gain, head_weight, clean, levels, table, gates, ids, w_gate, w_up,
         w_down):
    n_e, n_v = lax.axis_size("expert"), lax.axis_size("vocab")
    n_o, n_a = n_e // PAIR, n_v // CORES
    rows, width = layer_out.shape
    total_rows, share = rows * n_e, width // n_v
    vocab_local = head_weight.shape[1]
    local_experts, _, hidden = w_gate.shape
    lanes = -(-(local_experts * n_e + 2) // 128) * 128
    cut = share // 2
    dma = pltpu.SemaphoreType.DMA
    small = (layer_out, gain, clean, levels, table, gates, ids)
    buffers = [pltpu.VMEM(x.shape, x.dtype) for x in small] + [
        pltpu.VMEM((total_rows, width), bf16),
        pltpu.VMEM((total_rows, width), bf16),
        pltpu.VMEM((total_rows, width), bf16),
        pltpu.VMEM((total_rows, lanes), f32),
        pltpu.VMEM((lanes, 128), f32),
        pltpu.VMEM((width, vocab_local), bf16),
        pltpu.VMEM((n_a, share, vocab_local), bf16),
        pltpu.VMEM((width, 2 * local_experts * hidden), bf16),
        pltpu.VMEM((local_experts * hidden, width), bf16),
        pltpu.VMEM((total_rows, local_experts * hidden), f32),
        pltpu.VMEM((n_a, share, 2 * local_experts * hidden), bf16),
        pltpu.VMEM((total_rows, vocab_local), bf16),
        pltpu.VMEM((total_rows, vocab_local), bf16),
        pltpu.VMEM((total_rows, 2 * local_experts * hidden), bf16),
        pltpu.VMEM((total_rows, 2 * local_experts * hidden), bf16),
        pltpu.VMEM((n_a, 2, total_rows, cut), f32),
        pltpu.VMEM((local_experts, total_rows, hidden), f32),
        pltpu.VMEM((local_experts, total_rows, hidden), f32),
        pltpu.VMEM((2, 2, 2 * n_a - 1, n_o, rows, cut), bf16),
        pltpu.VMEM((2, 2, 2 * n_a - 1, n_o, rows, cut), bf16),
        pltpu.VMEM((2, n_o - 1, rows, cut), bf16),
        pltpu.VMEM((2, n_o - 1, rows, cut), bf16),
        pltpu.VMEM((2, n_o - 1, rows, cut), f32),
        pltpu.VMEM((2, n_o - 1, rows, cut), f32),
        pltpu.VMEM((2, rows, cut), f32),
        pltpu.VMEM((total_rows, 128), f32),
        pltpu.VMEM((3, 8, total_rows), f32),
        pltpu.VMEM((8, total_rows), f32),
        pltpu.VMEM((2 * n_a - 1, 8, total_rows), f32),
        pltpu.VMEM((n_o - 1, 8, total_rows), f32),
        pltpu.VMEM((rows, 128), f32),
        pltpu.VMEM((rows, width), f32),
    ]
    outs = [
        pltpu.VMEM((width, total_rows), bf16),
        pltpu.VMEM((total_rows, vocab_local), bf16),
        pltpu.VMEM((rows, share), f32),
        pltpu.VMEM((rows, share), f32),
    ]
    grant = VMEM_BYTES - sum(math.prod(x.shape) * jnp.dtype(x.dtype).itemsize for x in outs)
    scratch = buffers + [
        dma((KINDS, n_o - 1)), dma((KINDS, n_o)), dma((KINDS,)), dma((KINDS, 2)),
        dma((n_o - 1,)), dma((n_o,)), dma((3,)),
        dma((4,)), dma((4,)),
        dma((2, 4)), dma((2, 4)),
        dma((3,)), dma((3,)),
        dma((11,)),
    ]
    return pl.pallas_call(
        step_kernel,
        out_shape=outs,
        in_specs=[HBM] * 12,
        out_specs=[VMEM] * 4,
        scratch_shapes=scratch,
        compiler_params=pltpu.CompilerParams(
            collective_id=0, has_side_effects=True, vmem_limit_bytes=grant,
        ),
    )(layer_out, moe_input, gain, head_weight, clean, levels, table, gates, ids, w_gate, w_up,
      w_down)


def last_kernel(normed_ref, sg_ref, residual_ref, input_ref, head_grad, residual_out, input_out,
                tiles, sems):
    copies = [
        pltpu.make_async_copy(residual_ref, residual_out, sems.at[tiles.shape[0]]),
        pltpu.make_async_copy(input_ref, input_out, sems.at[tiles.shape[0] + 1]),
    ]
    for copy in copies:
        copy.start()
    tile = tiles.shape[1]
    for n in range(tiles.shape[0]):
        at = pl.ds(n * tile, tile)
        tiles[n] = jnp.dot(normed_ref[at, :], sg_ref[...], preferred_element_type=f32)
        copy = pltpu.make_async_copy(tiles.at[n], head_grad.at[at, :], sems.at[n])
        copy.start()
        copies.append(copy)
    for copy in copies:
        copy.wait()


def last(normed, sg, residual, input_grad):
    width = normed.shape[0]
    vocab_local = sg.shape[1]
    tiles = width // TILE
    return pl.pallas_call(
        last_kernel,
        out_shape=[
            jax.ShapeDtypeStruct((width, vocab_local), f32),
            jax.ShapeDtypeStruct(residual.shape, f32),
            jax.ShapeDtypeStruct(input_grad.shape, f32),
        ],
        in_specs=[VMEM] * 4,
        out_specs=[ANY] * 3,
        scratch_shapes=[
            pltpu.VMEM((tiles, TILE, vocab_local), f32),
            pltpu.SemaphoreType.DMA((tiles + 2,)),
        ],
        compiler_params=pltpu.CompilerParams(vmem_limit_bytes=4 * width * vocab_local + SPARE),
    )(*(pltpu.with_memory_space_constraint(x, pltpu.VMEM)
        for x in (normed, sg, residual, input_grad)))


def on_device(
    layer_out,
    moe_input,
    final_gain,
    head_weight,
    clean_ids,
    levels,
    ratio_table,
    gate_weights,
    expert_ids,
    w_gate,
    w_up,
    w_down,
):
    normed_all, score_grad, residual_grad, input_grad = step(
        layer_out, moe_input, final_gain[None, :], head_weight, clean_ids[None, :],
        levels[None, :], ratio_table[None, :], gate_weights.T, expert_ids.T, w_gate, w_up, w_down,
    )
    return tuple(last(normed_all, score_grad, residual_grad, input_grad))


def solution(mesh):
    in_specs = (
        P("expert", None),
        P("expert", None),
        P(),
        P(None, ("expert", "vocab")),
        P("expert"),
        P("expert"),
        P(),
        P("expert", None),
        P("expert", None),
        P("expert", None, "vocab"),
        P("expert", None, "vocab"),
        P("expert", "vocab", None),
    )
    out_specs = (P(None, ("expert", "vocab")), P("expert", "vocab"), P("expert", "vocab"))
    return jax.shard_map(
        on_device, mesh=mesh, in_specs=in_specs, out_specs=out_specs, check_vma=False
    )
```

```python
import functools
import math

import jax
import jax.numpy as jnp
from jax import lax
from jax.experimental import pallas as pl
from jax.experimental.pallas import tpu as pltpu
from jax.sharding import PartitionSpec as P

epsilon = 1e-05
CORES = 2
PAIR = 2
TILE = 256
SPARE = 6 << 20
VMEM_BYTES = 67043328
MESH = pl.DeviceIdType.MESH
ANY = pl.BlockSpec(memory_space=pl.ANY)
VMEM = pl.BlockSpec(memory_space=pltpu.VMEM)
HBM = pl.BlockSpec(memory_space=pltpu.HBM)
f32, bf16 = jnp.float32, jnp.bfloat16
TRANSPOSED = (((1,), (1,)), ((), ()))
NORMED, MOE, RES = range(3)
KINDS = 4
SG, HEAD, WEIGHTS, GRADS = range(4)


def flip(x, mask):
    bit = 1
    while bit <= mask:
        if mask & bit:
            x = x + bit - 2 * bit * ((x // bit) % 2)
        bit *= 2
    return x


def remote(src, dst, send, recv, target):
    return pltpu.make_async_remote_copy(
        src_ref=src, dst_ref=dst, send_sem=send, recv_sem=recv, device_id=target,
        device_id_type=MESH,
    )


def step_kernel(
    layer_hbm, moe_hbm, gain_hbm, head_hbm, clean_hbm, level_hbm, table_hbm, gates_hbm, ids_hbm,
    gate_hbm, up_hbm, down_hbm,
    normed_out, sg_out, residual_out, input_out,
    layer, gain, clean_ids, levels, table, gates, ids,
    normed_all, moe_all, res_all, meta_all, meta_t, head, head_pair, w_both, w_down, act,
    pair_both, sg, sg_pair, grads, grads_pair, part, fac_gate, fac_up,
    p_send, p_recv, z_send_0, z_recv_0, z_send_1, z_recv_1, own, dot_wide, dot_send, dot_recv, dot_chip, dot_outer, scale, unit,
    z_rs, plane_rs, sib_rs, out_ss, meta_z, meta_y, meta_one, one_ss, one_rs, rs_s, rs_r, dot_s,
    dot_r, local_sem,
):
    e, v = lax.axis_index("expert"), lax.axis_index("vocab")
    n_e, n_v = lax.axis_size("expert"), lax.axis_size("vocab")
    a, c, n_a = v // CORES, v % CORES, n_v // CORES
    o, i, n_o = e // PAIR, e % PAIR, n_e // PAIR
    rows, width = layer.shape
    total_rows = rows * n_e
    vocab_local = head_hbm.shape[1]
    local_experts, _, hidden = gate_hbm.shape
    experts_all = local_experts * n_e
    share = width // n_v
    cut = share // 2
    row_step = math.gcd(total_rows, 256)
    row_parts = [pl.ds(r, row_step) for r in range(0, total_rows, row_step)]

    def device(o_at, i_at, a_at):
        return (o_at * PAIR + i_at, a_at * CORES + c)

    sibling = (e, a * CORES + 1 - c)
    outer_peer = [device(flip(o, m), i, a) for m in range(n_o)]
    inner_peer = device(o, 1 - i, a)
    chip_at = [lax.rem(a + d, n_a) for d in range(n_a)]
    chip_from = [lax.rem(a + n_a - d, n_a) for d in range(n_a)]
    chip_peer = [device(o, i, chip_at[d]) for d in range(n_a)]
    diagonal_peer = [device(o, 1 - i, chip_at[d]) for d in range(n_a)]

    barrier = pltpu.get_barrier_semaphore()
    others = outer_peer[1:] + [inner_peer] + chip_peer[1:] + diagonal_peer[1:] + [sibling]
    for other in others:
        pl.semaphore_signal(barrier, inc=1, device_id=other, device_id_type=MESH)

    def block(m, across):
        at = flip(o, m) * PAIR + (1 - i if across else i)
        return pl.ds(pl.multiple_of(at * rows, rows), rows)

    def columns_of(at, core):
        return pl.ds(pl.multiple_of((at * CORES + core) * share, share), share)

    def cut_columns(at, s):
        return pl.ds(pl.multiple_of((at * CORES + c) * share + s * cut, cut), cut)

    def landed(ref, recv):
        remote(ref, ref, recv, recv, sibling).wait_recv()

    def left(ref, send):
        remote(ref, ref, send, send, sibling).wait_send()

    def piece(kind, buf, m, across, at, core):
        if kind >= RES:
            first = (at * CORES + core) * share + (kind - RES) * cut
            return buf.at[block(m, across), pl.ds(pl.multiple_of(first, cut), cut)]
        return buf.at[block(m, across), columns_of(at, core)]

    def post(kind, ref, recv, target, outer=False):
        remote(ref, ref, out_ss.at[kind, int(outer and kind >= RES)], recv, target).start()

    def plane(kind, buf, m):
        ref = piece(kind, buf, m, False, a, c)
        for d in range(1, n_a):
            if m or kind >= RES:
                post(kind, ref, plane_rs.at[kind, m], diagonal_peer[d])
            else:
                post(kind, piece(kind, buf, 0, False, chip_at[d], c), plane_rs.at[kind, m],
                     inner_peer)
            if m or kind >= RES:
                post(kind, ref, plane_rs.at[kind, m], chip_peer[d])
        post(kind, ref, plane_rs.at[kind, m], inner_peer)

    def to_sibling(kind, buf, m, across, d):
        post(kind, piece(kind, buf, m, across, chip_from[d], c), sib_rs.at[kind], sibling)

    def spread(kind, buf):
        ref = piece(kind, buf, 0, False, a, c)
        for m in range(1, n_o):
            post(kind, ref, z_rs.at[kind, m - 1], outer_peer[m], True)
        plane(kind, buf, 0)
        if kind >= RES:
            to_sibling(kind, buf, 0, False, 0)

    def forward(kind, buf, m):
        landed(piece(kind, buf, m, False, a, c), z_rs.at[kind, m - 1])
        plane(kind, buf, m)
        to_sibling(kind, buf, m, False, 0)

    def area(kind, buf, height, pieces):
        return buf.at[pl.ds(0, height * rows), pl.ds(0, pieces * (cut if kind >= RES else share))]

    def crossed(kind, buf, m):
        both = m > 0 or kind >= RES
        landed(area(kind, buf, 1, 2 * n_a - 1 if both else n_a), plane_rs.at[kind, m])
        to_sibling(kind, buf, m, True, 0)
        for across in ((False, True) if both else (True,)):
            for d in range(1, n_a):
                to_sibling(kind, buf, m, across, d)

    def from_sibling(kind, buf):
        landed(area(kind, buf, 2 * n_o if kind >= RES else 2 * n_o - 1, n_a), sib_rs.at[kind])

    def sent(kind, buf):
        if kind >= RES:
            left(area(kind, buf, n_o, 4 * n_a - 1), out_ss.at[kind, 0])
            left(area(kind, buf, n_o - 1, 1), out_ss.at[kind, 1])
        else:
            left(area(kind, buf, 2 * n_o - 1, 2 * n_a), out_ss.at[kind, 0])

    def lanes_of(k, j, n=1):
        return pl.ds((2 * k + j) * hidden, n * hidden)

    loads = [
        pltpu.make_async_copy(src, dst, local_sem.at[k])
        for k, (src, dst) in enumerate((
            (layer_hbm, layer), (gain_hbm, gain), (clean_hbm, clean_ids), (level_hbm, levels),
            (table_hbm, table), (gates_hbm, gates), (ids_hbm, ids), (head_hbm, head),
            (moe_hbm, moe_all.at[block(0, False)])))
    ]
    for copy in loads:
        copy.start()
    for k in range(local_experts):
        pltpu.make_async_copy(down_hbm.at[k], w_down.at[pl.ds(k * hidden, hidden), :],
                              local_sem.at[9]).start()
        for j, src in enumerate((gate_hbm, up_hbm)):
            pltpu.make_async_copy(src.at[k], w_both.at[:, lanes_of(k, j)], local_sem.at[10]).start()
    meta_t[...] = jnp.zeros_like(meta_t)
    for copy in loads[:7]:
        copy.wait()
    values = layer[...].astype(f32)
    row_scale = jnp.sqrt(jnp.sum(values * values, axis=1, keepdims=True) / width + epsilon)
    unit_rows = values / row_scale
    normed_all[block(0, False), :] = (unit_rows * gain[...]).astype(bf16)
    unit[...] = unit_rows
    scale[...] = jnp.broadcast_to(row_scale, scale.shape)
    label = lax.broadcasted_iota(jnp.int32, (experts_all, rows), 0)
    expert_gates = jnp.zeros((experts_all, rows), f32)
    for k in range(ids.shape[0]):
        expert_gates = expert_gates + jnp.where(ids[k:k + 1, :] == label, gates[k:k + 1, :], 0.0)
    ratio_row = jnp.zeros((1, rows), f32)
    for k in range(table.shape[1]):
        ratio_row = ratio_row + jnp.where(levels[...] == k, table[:, k:k + 1], 0.0)
    meta_t[0:experts_all, 0:rows] = expert_gates
    meta_t[experts_all:experts_all + 1, 0:rows] = ratio_row
    meta_t[experts_all + 1:experts_all + 2, 0:rows] = clean_ids[...].astype(f32)
    meta_all[block(0, False), :] = jnp.transpose(meta_t[...])[0:rows, :]
    pl.semaphore_wait(barrier, len(others))

    def meta_post(m, across, send, recv, target):
        ref = meta_all.at[block(m, across)]
        remote(ref, ref, meta_one.at[send], recv, target).start()

    @pl.when(c == CORES - 1)
    def _():
        for m in range(1, n_o):
            meta_post(0, False, 0, meta_z.at[m - 1], outer_peer[m])
        meta_post(0, False, 0, meta_y.at[0], inner_peer)
    spread(NORMED, normed_all)
    for d in range(n_a):
        theirs = columns_of(chip_at[d], 1 - c)
        remote(head_hbm.at[theirs, :], head_pair.at[d], one_ss.at[HEAD], one_rs.at[HEAD],
               sibling).start()
    for d in range(n_a):
        theirs = columns_of(chip_at[d], 1 - c)
        for k in range(local_experts):
            for j, src in enumerate((gate_hbm, up_hbm)):
                remote(src.at[k, theirs, :], pair_both.at[d, :, lanes_of(k, j)],
                       one_ss.at[WEIGHTS], one_rs.at[WEIGHTS], sibling).start()

    def factors(k):
        lane = lax.broadcasted_iota(jnp.int32, (1, meta_all.shape[1]), 1)
        for at in row_parts:
            x = moe_all[at, :]
            gate_pre = jnp.dot(x, w_both[:, lanes_of(k, 0)], preferred_element_type=f32)
            up_pre = jnp.dot(x, w_both[:, lanes_of(k, 1)], preferred_element_type=f32)
            weight = jnp.sum(jnp.where(lane == e * local_experts + k, meta_all[at, :], 0.0),
                             axis=1, keepdims=True)
            s = jax.nn.sigmoid(gate_pre)
            fac_gate[k, at, :] = weight * (up_pre * s * (1.0 + gate_pre * (1.0 - s)))
            fac_up[k, at, :] = weight * (gate_pre * s)

    act_seen = []

    def act_terms(s, core):
        for d in range(n_a):
            first = pl.multiple_of((chip_at[d] * CORES + core) * share + s * cut, cut)
            columns = pl.ds(first, cut)
            for at in row_parts:
                term = lax.dot_general(res_all[at, columns], w_down[:, columns], TRANSPOSED,
                                       preferred_element_type=f32)
                if act_seen:
                    act[at, :] += term
                else:
                    act[at, :] = term
            act_seen.append(d)

    def hidden_grads():
        for k in range(local_experts):
            for at in row_parts:
                own_act = act[at, pl.ds(k * hidden, hidden)]
                grads[at, lanes_of(k, 0)] = (own_act * fac_gate[k, at, :]).astype(bf16)
                grads[at, lanes_of(k, 1)] = (own_act * fac_up[k, at, :]).astype(bf16)

    def own_terms(q, d, s):
        columns = cut_columns(chip_at[d], s)
        left, right = (grads, w_both) if q else (sg, head)
        for at in row_parts:
            part[d, s, at, :] = lax.dot_general(left[at, :], right[columns, :], TRANSPOSED,
                                                preferred_element_type=f32)

    def pair_terms(q, d, s):
        columns = pl.ds(s * cut, cut)
        left, right = (grads_pair, pair_both) if q else (sg_pair, head_pair)
        for at in row_parts:
            part[d, s, at, :] += lax.dot_general(left[at, :], right[d, columns, :], TRANSPOSED,
                                                 preferred_element_type=f32)

    def scores():
        for at in row_parts:
            x = normed_all[at, :]
            meta = meta_all[at, :]
            ratio = meta[:, experts_all:experts_all + 1]
            clean = meta[:, experts_all + 1:experts_all + 2]
            score = jnp.dot(x, head[...], preferred_element_type=f32)
            label = (e * n_v + v) * vocab_local + lax.broadcasted_iota(
                jnp.int32, (1, vocab_local), 1)
            hit = jnp.where(clean == label.astype(f32), ratio, 0.0)
            grad = ((jnp.exp(score) - hit) * (1.0 / math.sqrt(total_rows))).astype(bf16)
            sg[at, :] = grad
            dot = jnp.sum(grad.astype(f32) * score, axis=1, keepdims=True)
            dot_wide[at, :] = jnp.broadcast_to(dot, (row_step, 128))
        dot_send[0] = jnp.transpose(dot_wide[...])[0:8, :]

    def exchange(q, stage, src, dst, target):
        remote(src, dst, rs_s.at[q, stage], rs_r.at[q, stage], target).start()

    z_send, z_recv = (z_send_0, z_send_1), (z_recv_0, z_recv_1)
    corners = [(d, across) for d in range(n_a) for across in (False, True) if d or across]
    corner_peer = [device(o, 1 - i if across else i, chip_at[d]) for d, across in corners]

    def terms_and_first(q):
        for s in range(2):
            for d in list(range(1, n_a)) + [0]:
                pair_terms(q, d, s)
                for j, (to, across) in enumerate(corners):
                    if to == d:
                        for m in range(n_o):
                            p_send[q, s, j, m] = part[d, s, block(m, across), :].astype(bf16)
                        exchange(q, s, p_send.at[q, s, j], p_recv.at[q, s, j], corner_peer[j])

    def dot_start(stage):
        src = dot_send.at[stage]
        if stage == 0:
            targets = [(dot_recv, sibling)]
        elif stage == 1:
            targets = [(dot_chip.at[j], peer) for j, peer in enumerate(corner_peer)]
        else:
            targets = [(dot_outer.at[m - 1], outer_peer[m]) for m in range(1, n_o)]
        for dst, target in targets:
            remote(src, dst, dot_s.at[stage], dot_r.at[stage], target).start()

    dot_whole = [dot_recv, dot_chip, dot_outer]

    def dot_sum(stage):
        landed(dot_whole[stage], dot_r.at[stage])
        total = dot_send[stage]
        if stage == 0:
            return total + dot_recv[...]
        for j in range(dot_whole[stage].shape[0]):
            total = total + dot_whole[stage][j]
        return total

    def dot_next(stage):
        dot_send[stage + 1] = dot_sum(stage)
        dot_start(stage + 1)

    def third(q):
        for s in range(2):
            landed(p_recv.at[q, s], rs_r.at[q, s])
            if q == 0 and s == 0:
                dot_next(1)
            for m in list(range(2, n_o)) + [1, 0]:
                term = part[0, s, block(m, False), :]
                for j in range(len(corners)):
                    term = term + p_recv[q, s, j, m].astype(f32)
                if m:
                    z_send[q][s, m - 1] = term.astype(z_send[q].dtype)
                    exchange(q, 2 + s, z_send[q].at[s, m - 1], z_recv[q].at[s, m - 1],
                             outer_peer[m])
                else:
                    own[s] = term

    def fourth(q, s):
        landed(z_recv[q].at[s], rs_r.at[q, 2 + s])
        term = own[s]
        for m in range(1, n_o):
            term = term + z_recv[q][s, m - 1].astype(f32)
        return term

    for m in range(1, n_o):
        @pl.when(c == CORES - 1)
        def _():
            landed(meta_all.at[block(m, False)], meta_z.at[m - 1])
            meta_post(m, False, 0, meta_y.at[m], inner_peer)
            meta_post(m, False, 1, meta_one.at[2], sibling)
        forward(NORMED, normed_all, m)
    loads[8].wait()
    spread(MOE, moe_all)
    for m in range(n_o):
        crossed(NORMED, normed_all, m)
        if m:
            forward(MOE, moe_all, m)
    meta_area = meta_all.at[pl.ds(0, (2 * n_o - 1) * rows)]

    @pl.when(c == CORES - 1)
    def _():
        for m in range(n_o):
            landed(meta_all.at[block(m, True)], meta_y.at[m])
            meta_post(m, True, 1, meta_one.at[2], sibling)
        left(meta_area, meta_one.at[0])
        left(meta_area, meta_one.at[1])

    @pl.when(c == 0)
    def _():
        landed(meta_area, meta_one.at[2])
    loads[7].wait()
    from_sibling(NORMED, normed_all)
    scores()
    remote(sg, sg_pair, one_ss.at[SG], one_rs.at[SG], sibling).start()
    dot_start(0)
    for s in range(2):
        for d in list(range(1, n_a)) + [0]:
            own_terms(0, d, s)
    landed(head_pair, one_rs.at[HEAD])
    landed(sg_pair, one_rs.at[SG])
    dot_next(0)
    terms_and_first(0)
    for at in row_parts:
        for n in range(0, width, row_step):
            normed_out[pl.ds(n, row_step), at] = jnp.transpose(normed_all[at, pl.ds(n, row_step)])
    sg_out[...] = sg[...]
    pltpu.make_async_copy(w_down, w_down, local_sem.at[9]).wait()
    pltpu.make_async_copy(w_both, w_both, local_sem.at[10]).wait()
    third(0)
    for m in range(n_o):
        crossed(MOE, moe_all, m)
    from_sibling(MOE, moe_all)
    dot_total = dot_sum(2)
    dot_wide[...] = jnp.transpose(jnp.broadcast_to(dot_total[0:1, :], (128, total_rows)))
    mean = dot_wide[block(0, False), 0:1] / width
    own_gain = gain[:, columns_of(a, c)]
    own_unit = unit[:, columns_of(a, c)]
    for s in range(2):
        at = slice(s * cut, (s + 1) * cut)
        residual = (own_gain[:, at] * fourth(0, s) - own_unit[:, at] * mean) / scale[:, 0:1]
        res_all[block(0, False), cut_columns(a, s)] = residual.astype(bf16)
        residual_out[:, at] = residual
        spread(RES + s, res_all)
        for k in range(s, local_experts, 2):
            factors(k)
    for s in range(2):
        for m in range(1, n_o):
            forward(RES + s, res_all, m)
    for s in range(2):
        for m in range(n_o):
            crossed(RES + s, res_all, m)
    from_sibling(RES, res_all)
    act_terms(0, c)
    act_terms(1, c)
    act_terms(0, 1 - c)
    from_sibling(RES + 1, res_all)
    act_terms(1, 1 - c)
    hidden_grads()
    remote(grads, grads_pair, one_ss.at[GRADS], one_rs.at[GRADS], sibling).start()
    for s in range(2):
        for d in list(range(1, n_a)) + [0]:
            own_terms(1, d, s)
    landed(pair_both, one_rs.at[WEIGHTS])
    landed(grads_pair, one_rs.at[GRADS])
    terms_and_first(1)
    third(1)
    for s in range(2):
        input_out[:, s * cut:(s + 1) * cut] = fourth(1, s)
    sent(NORMED, normed_all)
    sent(MOE, moe_all)
    for s in range(2):
        sent(RES + s, res_all)
    left(sg, one_ss.at[SG])
    left(head_pair, one_ss.at[HEAD])
    left(pair_both, one_ss.at[WEIGHTS])
    left(grads, one_ss.at[GRADS])
    for q in range(2):
        for s in range(2):
            left(p_send.at[q, s], rs_s.at[q, s])
            left(z_send[q].at[s], rs_s.at[q, 2 + s])
    for stage in range(3):
        left(dot_whole[stage], dot_s.at[stage])


def step(layer_out, moe_input, gain, head_weight, clean, levels, table, gates, ids, w_gate, w_up,
         w_down):
    n_e, n_v = lax.axis_size("expert"), lax.axis_size("vocab")
    n_o, n_a = n_e // PAIR, n_v // CORES
    rows, width = layer_out.shape
    total_rows, share = rows * n_e, width // n_v
    vocab_local = head_weight.shape[1]
    local_experts, _, hidden = w_gate.shape
    lanes = -(-(local_experts * n_e + 2) // 128) * 128
    cut = share // 2
    dma = pltpu.SemaphoreType.DMA
    small = (layer_out, gain, clean, levels, table, gates, ids)
    buffers = [pltpu.VMEM(x.shape, x.dtype) for x in small] + [
        pltpu.VMEM((total_rows, width), bf16),
        pltpu.VMEM((total_rows, width), bf16),
        pltpu.VMEM((total_rows, width), bf16),
        pltpu.VMEM((total_rows, lanes), f32),
        pltpu.VMEM((lanes, 128), f32),
        pltpu.VMEM((width, vocab_local), bf16),
        pltpu.VMEM((n_a, share, vocab_local), bf16),
        pltpu.VMEM((width, 2 * local_experts * hidden), bf16),
        pltpu.VMEM((local_experts * hidden, width), bf16),
        pltpu.VMEM((total_rows, local_experts * hidden), f32),
        pltpu.VMEM((n_a, share, 2 * local_experts * hidden), bf16),
        pltpu.VMEM((total_rows, vocab_local), bf16),
        pltpu.VMEM((total_rows, vocab_local), bf16),
        pltpu.VMEM((total_rows, 2 * local_experts * hidden), bf16),
        pltpu.VMEM((total_rows, 2 * local_experts * hidden), bf16),
        pltpu.VMEM((n_a, 2, total_rows, cut), f32),
        pltpu.VMEM((local_experts, total_rows, hidden), f32),
        pltpu.VMEM((local_experts, total_rows, hidden), f32),
        pltpu.VMEM((2, 2, 2 * n_a - 1, n_o, rows, cut), bf16),
        pltpu.VMEM((2, 2, 2 * n_a - 1, n_o, rows, cut), bf16),
        pltpu.VMEM((2, n_o - 1, rows, cut), bf16),
        pltpu.VMEM((2, n_o - 1, rows, cut), bf16),
        pltpu.VMEM((2, n_o - 1, rows, cut), f32),
        pltpu.VMEM((2, n_o - 1, rows, cut), f32),
        pltpu.VMEM((2, rows, cut), f32),
        pltpu.VMEM((total_rows, 128), f32),
        pltpu.VMEM((3, 8, total_rows), f32),
        pltpu.VMEM((8, total_rows), f32),
        pltpu.VMEM((2 * n_a - 1, 8, total_rows), f32),
        pltpu.VMEM((n_o - 1, 8, total_rows), f32),
        pltpu.VMEM((rows, 128), f32),
        pltpu.VMEM((rows, width), f32),
    ]
    outs = [
        pltpu.VMEM((width, total_rows), bf16),
        pltpu.VMEM((total_rows, vocab_local), bf16),
        pltpu.VMEM((rows, share), f32),
        pltpu.VMEM((rows, share), f32),
    ]
    grant = VMEM_BYTES - sum(math.prod(x.shape) * jnp.dtype(x.dtype).itemsize for x in outs)
    scratch = buffers + [
        dma((KINDS, n_o - 1)), dma((KINDS, n_o)), dma((KINDS,)), dma((KINDS, 2)),
        dma((n_o - 1,)), dma((n_o,)), dma((3,)),
        dma((4,)), dma((4,)),
        dma((2, 4)), dma((2, 4)),
        dma((3,)), dma((3,)),
        dma((11,)),
    ]
    return pl.pallas_call(
        step_kernel,
        out_shape=outs,
        in_specs=[HBM] * 12,
        out_specs=[VMEM] * 4,
        scratch_shapes=scratch,
        compiler_params=pltpu.CompilerParams(
            collective_id=0, has_side_effects=True, vmem_limit_bytes=grant,
        ),
    )(layer_out, moe_input, gain, head_weight, clean, levels, table, gates, ids, w_gate, w_up,
      w_down)


def last_kernel(normed_ref, sg_ref, residual_ref, input_ref, head_grad, residual_out, input_out,
                tiles, sems):
    copies = [
        pltpu.make_async_copy(residual_ref, residual_out, sems.at[tiles.shape[0]]),
        pltpu.make_async_copy(input_ref, input_out, sems.at[tiles.shape[0] + 1]),
    ]
    for copy in copies:
        copy.start()
    tile = tiles.shape[1]
    for n in range(tiles.shape[0]):
        at = pl.ds(n * tile, tile)
        tiles[n] = jnp.dot(normed_ref[at, :], sg_ref[...], preferred_element_type=f32)
        copy = pltpu.make_async_copy(tiles.at[n], head_grad.at[at, :], sems.at[n])
        copy.start()
        copies.append(copy)
    for copy in copies:
        copy.wait()


def last(normed, sg, residual, input_grad):
    width = normed.shape[0]
    vocab_local = sg.shape[1]
    tiles = width // TILE
    return pl.pallas_call(
        last_kernel,
        out_shape=[
            jax.ShapeDtypeStruct((width, vocab_local), f32),
            jax.ShapeDtypeStruct(residual.shape, f32),
            jax.ShapeDtypeStruct(input_grad.shape, f32),
        ],
        in_specs=[VMEM] * 4,
        out_specs=[ANY] * 3,
        scratch_shapes=[
            pltpu.VMEM((tiles, TILE, vocab_local), f32),
            pltpu.SemaphoreType.DMA((tiles + 2,)),
        ],
        compiler_params=pltpu.CompilerParams(vmem_limit_bytes=4 * width * vocab_local + SPARE),
    )(*(pltpu.with_memory_space_constraint(x, pltpu.VMEM)
        for x in (normed, sg, residual, input_grad)))


def on_device(
    layer_out,
    moe_input,
    final_gain,
    head_weight,
    clean_ids,
    levels,
    ratio_table,
    gate_weights,
    expert_ids,
    w_gate,
    w_up,
    w_down,
):
    normed_all, score_grad, residual_grad, input_grad = step(
        layer_out, moe_input, final_gain[None, :], head_weight, clean_ids[None, :],
        levels[None, :], ratio_table[None, :], gate_weights.T, expert_ids.T, w_gate, w_up, w_down,
    )
    return tuple(last(normed_all, score_grad, residual_grad, input_grad))


def solution(mesh):
    in_specs = (
        P("expert", None),
        P("expert", None),
        P(),
        P(None, ("expert", "vocab")),
        P("expert"),
        P("expert"),
        P(),
        P("expert", None),
        P("expert", None),
        P("expert", None, "vocab"),
        P("expert", None, "vocab"),
        P("expert", "vocab", None),
    )
    out_specs = (P(None, ("expert", "vocab")), P("expert", "vocab"), P("expert", "vocab"))
    return jax.shard_map(
        on_device, mesh=mesh, in_specs=in_specs, out_specs=out_specs, check_vma=False
    )
```
